32 devices in a mesh: rows: 8 (over z, x), cols: 4 (over y, core).
Axes of the slice: x: 2, y: 2, z: 4, core: 2. Of those that a mesh axis runs over, the one named last changes fastest.
Arguments:
- panel: float32 [4096, 1024], P('rows'), as said below
- window_block: float32 [4096, 2048], P('rows', 'cols'), may hold values from -6 to 6
- row_live: int32 [8], replicated, may hold values 0 or 1
- window_rows: int32 [4], replicated, may hold values from 2 to 7, as said below
Outputs:
- factor: float32 [4096, 1024], P('rows')
- updated: float32 [4096, 2048], P('rows', 'cols')
The draws below stay inside these ranges and needn't reach their ends.
Inputs may be any that keep to these rules, and one draw needn't show every extreme that they name: `window_rows`: distinct tile rows, none inside the supernode. `row_live`: the value for tile rows below 2 is ignored: those rows are always present. `panel`: the first 1024 rows hold a symmetric positive definite block.
All inputs are finite; a program needn't handle non-finite values.
Results may differ from the reference program's by a relative error of at most 0.0001.
Values sent between devices are 32-bit elements; how exact they have to be, the bound alone decides.
A program may use at most 128 MiB of HBM per device.

```python
import jax
import jax.numpy as jnp
from jax import lax

B = 512
P_SIZE = 2
NT = 8
NW = 4


def draw_window_rows(key, part):
    pair = jax.random.split(key, 2)
    first = jax.random.randint(pair[0], (NT - P_SIZE,), 0, 1 << 14)
    second = jax.random.randint(pair[1], (NT - P_SIZE,), 0, 1 << 14)
    scores = (first * 16384 + second) % 1048576
    distinct = scores * NT + jnp.arange(NT - P_SIZE)
    values, places = lax.top_k(distinct, NW)
    return (places + P_SIZE).astype(jnp.int32)


def draw_panel(key, part):
    keys = jax.random.split(jax.random.fold_in(key, 5), 5)
    total_rows = NT * B
    width = P_SIZE * B
    reach = max(4.0, width / 48.0)
    base = jax.random.normal(keys[0], (total_rows, width)) * 0.25
    rough = jax.random.normal(keys[1], (width, width)) * (0.15 / width ** 0.5)
    rough = (rough + rough.T) * 0.70710678
    places = jnp.arange(width).astype(jnp.float32)
    distance = jnp.abs(places[:, None] - places[None, :])
    kernel = 0.6 * jnp.exp(-distance / reach)
    diag_vals = jax.random.uniform(keys[2], (width,), minval=0.8, maxval=1.6)
    scales = jnp.exp(jax.random.uniform(keys[4], (width,), minval=jnp.log(0.8), maxval=jnp.log(1.25)))
    head = scales[:, None] * scales[None, :] * (kernel + rough) + jnp.diag(diag_vals)
    head_full = jnp.concatenate([head, jnp.zeros((total_rows - width, width), jnp.float32)], axis=0)
    row_ids = jnp.arange(total_rows)[:, None]
    return jnp.where(row_ids < width, head_full, base).astype(jnp.float32)


def set_ends(array, stream_key, smallest, largest):
    extent = array.shape
    place = [jax.random.randint(jax.random.fold_in(stream_key, axis), (), 0, extent[axis]) for axis in range(len(extent))]
    array = array.at[tuple(place)].set(smallest)
    longest = extent.index(max(extent))
    place[longest] = (place[longest] + 1) % extent[longest]
    return array.at[tuple(place)].set(largest)


def block_levels(rng, shape, pieces, low, largest):
    loudness, own = 1.0, jax.random.fold_in(rng, 6)
    for position, blocks in pieces:
        draws = jnp.exp(jax.random.uniform(jax.random.fold_in(own, position), (blocks,), jnp.float32, low / len(pieces), largest / len(pieces)))
        loudness = loudness * jnp.repeat(draws, shape[position] // blocks).reshape([-1 if axis == position else 1 for axis in range(len(shape))])
    return loudness


def noise(rng, extent, spread, most, cuts=(), dtype=jnp.bfloat16):
    result = spread * jax.random.normal(rng, extent, jnp.float32)
    if cuts:
        result = result * block_levels(rng, extent, cuts, -0.22, 0.18)
    return jnp.clip(result, -most, most).astype(dtype)


def setup_inputs(seed: int = 0) -> dict:
    arg_keys = jax.random.split(jax.random.key(seed), 5)
    return {
        "panel": draw_panel(jax.random.fold_in(arg_keys[4], 71), 0),
        "window_block": noise(arg_keys[1], (NT * B, NW * B), 1.0, 6.0, ((0, 8), (1, 4)), jnp.float32),
        "row_live": set_ends((jax.random.randint(arg_keys[2], (NT,), 0, 4) < 3).astype(jnp.int32), jax.random.fold_in(arg_keys[2], 1), 0, 1),
        "window_rows": draw_window_rows(jax.random.fold_in(arg_keys[4], 71), 0),
    }


def reference(panel, window_block, row_live, window_rows):
    tile_ids = jnp.arange(NT)
    live_flag = jnp.where(tile_ids < P_SIZE, 1, row_live).astype(jnp.float32)
    scaled = panel * jnp.repeat(live_flag, B)[:, None]
    head = scaled[:P_SIZE * B]
    square = jnp.tril(head) + jnp.tril(head, -1).T
    lower = jnp.linalg.cholesky(square)
    solved = lax.linalg.triangular_solve(lower, scaled, left_side=False, lower=True, transpose_a=True)
    factor = jnp.concatenate([lower, solved[P_SIZE * B:]], axis=0)
    columns = []
    for window in range(NW):
        start = (window_rows[window] * B).astype(jnp.int32)
        target_row = lax.dynamic_slice_in_dim(factor, start, B, 0)
        block_now = window_block[:, window * B:(window + 1) * B]
        product = lax.dot_general(factor, target_row, (((1,), (1,)), ((), ())), precision=lax.Precision.HIGHEST)
        columns.append(block_now - product)
    return (factor, jnp.concatenate(columns, axis=1))
```

```python
import functools

import jax
import jax.numpy as jnp
from jax import lax
from jax.experimental import pallas as pl
from jax.experimental.pallas import tpu as pltpu
from jax.sharding import PartitionSpec as P

P_SIZE = 2
HIGHEST = lax.Precision.HIGHEST
CONTRACT = (((1,), (1,)), ((), ()))
PLAIN = (((1,), (0,)), ((), ()))
LEAF = 128
GROUP = 16
WIDE = 256
MESH = pl.DeviceIdType.MESH


def halves(value):
    high = value.astype(jnp.bfloat16)
    return high, (value - high.astype(jnp.float32)).astype(jnp.bfloat16)


def product(left, right, contract):
    lh, ll = halves(left)
    rh, rl = halves(right)

    def dot(a, b):
        return lax.dot_general(a, b, contract, preferred_element_type=jnp.float32)

    return dot(lh, rh) + (dot(lh, rl) + dot(ll, rh))


def times_trans(left, right):
    return product(left, right, CONTRACT)


def times(left, right):
    return product(left, right, PLAIN)


def spread_kernel(n_rows, panel, first, second, row_send, row_recv, far_send, far_recv, near_send, near_recv):
    r = lax.axis_index("rows")
    c = lax.axis_index("cols")
    far = lax.rem(c + 2, 4)
    near = c + 1 - 2 * lax.rem(c, 2)
    width = panel.shape[0]
    n_blocks = width // LEAF
    share = LEAF // 4
    pieces = [(which, b) for which in range(2) for b in range(n_blocks)]

    barrier = pltpu.get_barrier_semaphore()
    for other in (far, near):
        pl.semaphore_signal(barrier, inc=1, device_id=(r, other), device_id_type=MESH)

    @pl.when(r < 2)
    def _():
        pl.semaphore_signal(barrier, inc=1, device_id=(1 - r, c), device_id_type=MESH)

    @pl.when(r >= 2)
    def _():
        pl.semaphore_signal(barrier, inc=1, device_id=(r - 2, c), device_id_type=MESH)

    @pl.when(r + 2 < n_rows)
    def _():
        pl.semaphore_signal(barrier, inc=1, device_id=(r + 2, c), device_id_type=MESH)

    pl.semaphore_wait(barrier, 3 + (r + 2 < n_rows).astype(jnp.int32))

    def window(ref, piece, owner):
        which, b = pieces[piece]
        start = pl.multiple_of(b * LEAF + owner * share, 8)
        return ref.at[pl.ds(start, share), pl.ds(0, which * width + (b + 1) * LEAF)]

    def landing(piece, owner):
        return window((first, second)[pieces[piece][0]], piece, owner)

    def to_row(piece, slot, dest, own):
        return pltpu.make_async_remote_copy(
            src_ref=window(panel, piece, c) if own else landing(piece, c), dst_ref=landing(piece, c),
            send_sem=row_send.at[piece, slot], recv_sem=row_recv.at[piece],
            device_id=(dest, c), device_id_type=MESH)

    def to_far(piece):
        return pltpu.make_async_remote_copy(
            src_ref=landing(piece, c), dst_ref=landing(piece, c),
            send_sem=far_send.at[piece], recv_sem=far_recv.at[piece],
            device_id=(r, far), device_id_type=MESH)

    def to_near(piece, slot):
        owner = (c, far)[slot]
        return pltpu.make_async_remote_copy(
            src_ref=landing(piece, owner), dst_ref=landing(piece, owner),
            send_sem=near_send.at[piece, slot], recv_sem=near_recv.at[piece, slot],
            device_id=(r, near), device_id_type=MESH)

    for piece in range(len(pieces)):
        which = pieces[piece][0]

        @pl.when(r == which)
        def _():
            to_row(piece, 0, 1 - which, True).start()
            if which + 2 < n_rows:
                to_row(piece, 1, which + 2, True).start()

    @pl.when(r == 0)
    def _():
        first[...] = panel[:, :width]

    @pl.when(r == 1)
    def _():
        second[...] = panel[...]

    for piece in range(len(pieces) + 1):
        if piece < len(pieces):

            @pl.when(r != pieces[piece][0])
            def _():
                to_row(piece, 0, r, False).wait_recv()

                @pl.when(r + 2 < n_rows)
                def _():
                    to_row(piece, 0, r + 2, False).start()

                to_far(piece).start()
                to_near(piece, 0).start()

        if piece > 0:

            @pl.when(r != pieces[piece - 1][0])
            def _():
                to_far(piece - 1).wait_recv()
                to_near(piece - 1, 1).start()

    for piece in range(len(pieces)):
        which = pieces[piece][0]

        @pl.when(r != which)
        def _():
            for slot in range(2):
                to_near(piece, slot).wait_recv()
            for slot in range(2):
                to_near(piece, slot).wait_send()
            to_far(piece).wait_send()

            @pl.when(r + 2 < n_rows)
            def _():
                to_row(piece, 0, r + 2, False).wait_send()

        @pl.when(r == which)
        def _():
            to_row(piece, 0, 1 - which, True).wait_send()
            if which + 2 < n_rows:
                to_row(piece, 1, which + 2, True).wait_send()


def split3(value):
    high = value.astype(jnp.bfloat16).astype(jnp.float32)
    rest = value - high
    mid = rest.astype(jnp.bfloat16).astype(jnp.float32)
    return high, mid, rest - mid


def factor_leaf(aug, upper, inverse):
    lanes = lax.broadcasted_iota(jnp.int32, (GROUP, LEAF), 1)
    subs = lax.broadcasted_iota(jnp.int32, (GROUP, LEAF), 0)
    for g in range(LEAF // GROUP):
        base = g * GROUP
        left = aug[base : base + GROUP, :LEAF]
        right = aug[base : base + GROUP, LEAF:]
        cols = [
            jnp.broadcast_to(left[:, base + j : base + j + 1], (GROUP, LEAF)) for j in range(GROUP)
        ]
        scale = jnp.zeros((GROUP, LEAF), jnp.float32)
        for k in range(GROUP):
            pivot = jnp.broadcast_to(cols[k][k : k + 1, :], (GROUP, LEAF))
            root = lax.rsqrt(pivot)
            scale = jnp.where(subs == k, root, scale)
            if k + 1 < GROUP:
                mult = jnp.where(subs > k, cols[k] * (root * root), 0.0)
                for j in range(k + 1, GROUP):
                    cols[j] = cols[j] - mult * jnp.broadcast_to(cols[j][k : k + 1, :], (GROUP, LEAF))
                left = left - mult * jnp.broadcast_to(left[k : k + 1, :], (GROUP, LEAF))
                right = right - mult * jnp.broadcast_to(right[k : k + 1, :], (GROUP, LEAF))
        row_of = lanes - base
        left = jnp.where(row_of >= subs, left * scale, 0.0)
        right = right * scale
        upper[base : base + GROUP, :] = left
        inverse[base : base + GROUP, :] = right
        if base + GROUP < LEAF:
            lh, lm, ll = split3(left)
            rh, rm, rl = split3(right)
            keep = lanes >= base + GROUP
            a = [jnp.where(keep, v, 0.0) for v in (lh, lm, ll)]
            lhs = jnp.concatenate([a[0], a[0], a[1], a[0], a[1], a[2]], axis=0)
            rl_ = jnp.concatenate([lh, lm, lh, ll, lm, lh], axis=0)
            rr_ = jnp.concatenate([rh, rm, rh, rl, rm, rh], axis=0)
            rhs = jnp.concatenate([rl_, rr_], axis=1)
            update = lax.dot_general(
                lhs, rhs, (((0,), (0,)), ((), ())), preferred_element_type=jnp.float32)
            aug[base + GROUP :, :] = aug[base + GROUP :, :] - update[base + GROUP :, :]


def factor_kernel(live, first, second, panel, factor, solved, lower, inverses, aug, upper, leaf_inv):
    width = first.shape[0]
    total = lower.shape[0]
    n_leaf = total // LEAF
    per = width // LEAF
    rows = lax.broadcasted_iota(jnp.int32, (LEAF, LEAF), 0)
    lanes = lax.broadcasted_iota(jnp.int32, (LEAF, LEAF), 1)
    lower[:width, :width] = first[...]
    lower[:width, width:] = jnp.zeros((width, total - width), jnp.float32)
    lower[width:, :] = second[...]
    for b in range(n_leaf - 1):
        lower[b * LEAF : (b + 1) * LEAF, (b + 1) * LEAF :] = jnp.zeros(
            (LEAF, total - (b + 1) * LEAF), jnp.float32)
    inverses[...] = jnp.zeros(inverses.shape, jnp.float32)

    def step(k, carry):
        at = pl.ds(pl.multiple_of(k * LEAF, LEAF), LEAF)
        block = lower[at, at]
        aug[:, :LEAF] = jnp.where(rows >= lanes, block, block.T)
        aug[:, LEAF:] = jnp.where(rows == lanes, 1.0, 0.0)
        factor_leaf(aug, upper, leaf_inv)
        lower[at, at] = upper[...].T
        for b in range(n_leaf):

            @pl.when(k == b)
            def _():
                lo, hi = b * LEAF, (b + 1) * LEAF
                wide = b * LEAF // WIDE
                off = lo - wide * WIDE
                inv = leaf_inv[...]
                inverses[wide, off : off + LEAF, off : off + LEAF] = inv
                if off:
                    before = inverses[wide, :LEAF, :LEAF]
                    cross = lower[lo:hi, lo - LEAF : lo]
                    part = lax.dot_general(
                        cross, before, (((1,), (0,)), ((), ())), precision=HIGHEST,
                        preferred_element_type=jnp.float32)
                    inverses[wide, LEAF:, :LEAF] = -lax.dot_general(
                        inv, part, (((1,), (0,)), ((), ())), precision=HIGHEST,
                        preferred_element_type=jnp.float32)
                if hi < total:
                    lower[hi:, lo:hi] = times_trans(lower[hi:, lo:hi], inv)
                    nxt = hi + LEAF
                    lower[hi:, hi:nxt] = lower[hi:, hi:nxt] - times_trans(
                        lower[hi:, :hi], lower[hi:nxt, :hi])

        return carry

    lax.fori_loop(0, n_leaf, step, 0)

    r = lax.axis_index("rows")
    n_wide = total // WIDE

    @pl.when(r < P_SIZE)
    def _():
        factor[...] = lower[pl.ds(pl.multiple_of(lax.rem(r, P_SIZE) * width, width), width), :]

    @pl.when(r >= P_SIZE)
    def _():
        factor[...] = panel[...] * live[0]
        for wide in range(n_wide):
            lo, hi = wide * WIDE, (wide + 1) * WIDE
            now = factor[:, lo:hi]
            if wide:
                now = now - times_trans(factor[:, :lo], lower[lo:hi, :lo])
            factor[:, lo:hi] = times_trans(now, inverses[wide])

    for wide in reversed(range(n_wide)):
        lo, hi = wide * WIDE, (wide + 1) * WIDE
        now = factor[:, lo:hi]
        if hi < total:
            now = now - times(solved[:, hi:], lower[hi:, lo:hi])
        solved[:, lo:hi] = times(now, inverses[wide])


def fused_kernel(n_rows, live, panel, factor, solved, first, second, lower, inverses, aug, upper, leaf_inv, *sems):
    spread_kernel(n_rows, panel, first, second, *sems)
    factor_kernel(live, first, second, panel, factor, solved, lower, inverses, aug, upper, leaf_inv)


def factor_rows(live, panel, n_rows, n_cols):
    width = panel.shape[0]
    n_pieces = 2 * (width // LEAF)
    total = P_SIZE * width
    return pl.pallas_call(
        functools.partial(fused_kernel, n_rows),
        out_shape=(jax.ShapeDtypeStruct(panel.shape, jnp.float32),) * 2,
        in_specs=[pl.BlockSpec(memory_space=pltpu.SMEM)] + [pl.BlockSpec(memory_space=pltpu.VMEM)],
        out_specs=(pl.BlockSpec(memory_space=pltpu.VMEM),) * 2,
        scratch_shapes=[
            pltpu.VMEM((width, width), jnp.float32),
            pltpu.VMEM((width, total), jnp.float32),
            pltpu.VMEM((total, total), jnp.float32),
            pltpu.VMEM((total // WIDE, WIDE, WIDE), jnp.float32),
            pltpu.VMEM((LEAF, 2 * LEAF), jnp.float32),
            pltpu.VMEM((LEAF, LEAF), jnp.float32),
            pltpu.VMEM((LEAF, LEAF), jnp.float32),
            pltpu.SemaphoreType.DMA((n_pieces, 2)),
            pltpu.SemaphoreType.DMA((n_pieces,)),
            pltpu.SemaphoreType.DMA((n_pieces,)),
            pltpu.SemaphoreType.DMA((n_pieces,)),
            pltpu.SemaphoreType.DMA((n_pieces, 2)),
            pltpu.SemaphoreType.DMA((n_pieces, 2)),
        ],
        compiler_params=pltpu.CompilerParams(collective_id=0, has_side_effects=True, vmem_limit_bytes=40 << 20),
        cost_estimate=pl.CostEstimate(flops=10**10, bytes_accessed=10**7, transcendentals=0),
        name="factor_rows",
    )(live, panel)


def update_kernel(solved, target, window, updated):
    updated[...] = window[...] - times_trans(solved[...], target[...])


def update_window(solved, target, window):
    return pl.pallas_call(
        update_kernel,
        out_shape=jax.ShapeDtypeStruct(window.shape, jnp.float32),
        in_specs=[pl.BlockSpec(memory_space=pltpu.VMEM)] * 3,
        out_specs=pl.BlockSpec(memory_space=pltpu.VMEM),
        compiler_params=pltpu.CompilerParams(vmem_limit_bytes=40 << 20),
        cost_estimate=pl.CostEstimate(flops=10**9, bytes_accessed=10**7, transcendentals=0),
        name="update_window",
    )(solved, target, window)


def shards(n_rows, n_cols, panel, window_block, row_live, window_rows):
    device_row = lax.axis_index("rows")
    device_col = lax.axis_index("cols")
    live = jnp.where(device_row < P_SIZE, 1, row_live[device_row]).astype(jnp.float32)
    target = window_rows[device_col]
    kept = jnp.where(device_row == target, panel * live, 0)
    kept, panel = lax.optimization_barrier((kept, panel))
    target_raw = lax.psum(kept, "rows")
    factor, solved = factor_rows(live[None], panel, n_rows, n_cols)
    updated = update_window(solved, target_raw, window_block)
    return (factor, updated)


def solution(mesh):
    in_specs = (P("rows", None), P("rows", "cols"), P(), P())
    out_specs = (P("rows", None), P("rows", "cols"))
    body = functools.partial(shards, mesh.shape["rows"], mesh.shape["cols"])
    return jax.shard_map(body, mesh=mesh, in_specs=in_specs, out_specs=out_specs, check_vma=False)
```

```python
import functools

import jax
import jax.numpy as jnp
from jax import lax
from jax.experimental import pallas as pl
from jax.experimental.pallas import tpu as pltpu
from jax.sharding import PartitionSpec as P

P_SIZE = 2
HIGHEST = lax.Precision.HIGHEST
CONTRACT = (((1,), (1,)), ((), ()))
PLAIN = (((1,), (0,)), ((), ()))
LEAF = 128
GROUP = 16
WIDE = 256
MESH = pl.DeviceIdType.MESH


def halves(value):
    high = value.astype(jnp.bfloat16)
    return high, (value - high.astype(jnp.float32)).astype(jnp.bfloat16)


def product(left, right, contract):
    lh, ll = halves(left)
    rh, rl = halves(right)

    def dot(a, b):
        return lax.dot_general(a, b, contract, preferred_element_type=jnp.float32)

    return dot(lh, rh) + (dot(lh, rl) + dot(ll, rh))


def times_trans(left, right):
    return product(left, right, CONTRACT)


def times(left, right):
    return product(left, right, PLAIN)


def split3(value):
    high = value.astype(jnp.bfloat16).astype(jnp.float32)
    rest = value - high
    mid = rest.astype(jnp.bfloat16).astype(jnp.float32)
    return high, mid, rest - mid


def factor_leaf(aug, upper, inverse):
    lanes = lax.broadcasted_iota(jnp.int32, (GROUP, LEAF), 1)
    subs = lax.broadcasted_iota(jnp.int32, (GROUP, LEAF), 0)
    for g in range(LEAF // GROUP):
        base = g * GROUP
        left = aug[base : base + GROUP, :LEAF]
        right = aug[base : base + GROUP, LEAF:]
        cols = [
            jnp.broadcast_to(left[:, base + j : base + j + 1], (GROUP, LEAF)) for j in range(GROUP)
        ]
        scale = jnp.zeros((GROUP, LEAF), jnp.float32)
        for k in range(GROUP):
            pivot = jnp.broadcast_to(cols[k][k : k + 1, :], (GROUP, LEAF))
            root = lax.rsqrt(pivot)
            scale = jnp.where(subs == k, root, scale)
            if k + 1 < GROUP:
                mult = jnp.where(subs > k, cols[k] * (root * root), 0.0)
                for j in range(k + 1, GROUP):
                    cols[j] = cols[j] - mult * jnp.broadcast_to(cols[j][k : k + 1, :], (GROUP, LEAF))
                left = left - mult * jnp.broadcast_to(left[k : k + 1, :], (GROUP, LEAF))
                right = right - mult * jnp.broadcast_to(right[k : k + 1, :], (GROUP, LEAF))
        row_of = lanes - base
        left = jnp.where(row_of >= subs, left * scale, 0.0)
        right = right * scale
        upper[base : base + GROUP, :] = left
        inverse[base : base + GROUP, :] = right
        if base + GROUP < LEAF:
            lh, lm, ll = split3(left)
            rh, rm, rl = split3(right)
            keep = lanes >= base + GROUP
            a = [jnp.where(keep, v, 0.0) for v in (lh, lm, ll)]
            lhs = jnp.concatenate([a[0], a[0], a[1], a[0], a[1], a[2]], axis=0)
            rl_ = jnp.concatenate([lh, lm, lh, ll, lm, lh], axis=0)
            rr_ = jnp.concatenate([rh, rm, rh, rl, rm, rh], axis=0)
            rhs = jnp.concatenate([rl_, rr_], axis=1)
            update = lax.dot_general(
                lhs, rhs, (((0,), (0,)), ((), ())), preferred_element_type=jnp.float32)
            aug[base + GROUP :, :] = aug[base + GROUP :, :] - update[base + GROUP :, :]


CHUNKS = 4


class Traffic:
    def __init__(self, n_rows, n_cols, panel, own, lower, target, gathered, staged, sems):
        self.n_rows, self.n_cols = n_rows, n_cols
        self.n_pos = n_rows // 2
        self.r = lax.axis_index("rows")
        self.c = lax.axis_index("cols")
        self.q = lax.div(self.r, 2)
        self.p = lax.rem(self.r, 2)
        self.partner = self.r + 1 - 2 * self.p
        self.far = lax.rem(self.c + 2, 4)
        self.near = self.c + 1 - 2 * lax.rem(self.c, 2)
        self.panel, self.own, self.lower, self.target = panel, own, lower, target
        self.gathered, self.staged = gathered, staged
        (self.row_send, self.row_recv, self.far_send, self.far_recv, self.near_send, self.near_recv,
         self.dn_send, self.dn_recv, self.up_send, self.up_recv, self.x_send, self.x_recv,
         self.t_send, self.t_recv) = sems
        self.width = panel.shape[0]
        self.share = self.width // n_cols
        self.chunk = self.share // CHUNKS
        per = self.width // LEAF
        self.columns = []
        self.pieces = []
        for k in range(2 * per):
            column = []
            for which in range(2):
                lo = max(0, k - which * per) * LEAF
                if lo < self.width:
                    column.append(len(self.pieces))
                    self.pieces.append((which, lo, self.width - lo, k))
            self.columns.append(column)

    def barrier(self):
        sem = pltpu.get_barrier_semaphore()
        r, c, q = self.r, self.c, self.q

        def greet(row, col):
            pl.semaphore_signal(sem, inc=1, device_id=(row, col), device_id_type=MESH)

        for i in range(1, self.n_cols):
            greet(r, lax.rem(c + i, self.n_cols))
        greet(self.partner, c)

        @pl.when(q >= 1)
        def _():
            greet(r - 2, c)

        @pl.when(q + 1 < self.n_pos)
        def _():
            greet(r + 2, c)

        count = self.n_cols + (q >= 1).astype(jnp.int32) + (q + 1 < self.n_pos).astype(jnp.int32)
        pl.semaphore_wait(sem, count)

    def remote(self, src, dst, send, recv, row, col):
        return pltpu.make_async_remote_copy(
            src_ref=src, dst_ref=dst, send_sem=send, recv_sem=recv,
            device_id=(row, col), device_id_type=MESH)

    def place(self, ref, piece, owner):
        which, lo, size, k = self.pieces[piece]
        base = which * self.width if ref is self.lower else 0
        start = pl.multiple_of(base + lo + owner * (size // 4), 8)
        return ref.at[pl.ds(start, size // 4), pl.ds(k * LEAF, LEAF)]

    def to_row(self, piece, slot, dest, own):
        src = self.place(self.panel if own else self.lower, piece, self.c)
        return self.remote(src, self.place(self.lower, piece, self.c),
                           self.row_send.at[piece, slot], self.row_recv.at[piece], dest, self.c)

    def to_far(self, piece):
        spot = self.place(self.lower, piece, self.c)
        return self.remote(spot, spot, self.far_send.at[piece], self.far_recv.at[piece], self.r, self.far)

    def to_near(self, piece, slot):
        spot = self.place(self.lower, piece, (self.c, self.far)[slot])
        return self.remote(spot, spot, self.near_send.at[piece, slot], self.near_recv.at[piece, slot],
                           self.r, self.near)

    def send_diagonal(self):
        for piece, (which, _, _, _) in enumerate(self.pieces):

            @pl.when(self.r == which)
            def _():
                self.to_row(piece, 0, 1 - which, True).start()
                if which + 2 < self.n_rows:
                    self.to_row(piece, 1, which + 2, True).start()

    def column_in(self, k):
        for piece in self.columns[k]:

            @pl.when(self.r != self.pieces[piece][0])
            def _():
                self.to_row(piece, 0, self.r, False).wait_recv()

                @pl.when(self.r + 2 < self.n_rows)
                def _():
                    self.to_row(piece, 0, self.r + 2, False).start()

                self.to_far(piece).start()
                self.to_near(piece, 0).start()

    def column_far(self, k):
        for piece in self.columns[k]:

            @pl.when(self.r != self.pieces[piece][0])
            def _():
                self.to_far(piece).wait_recv()
                self.to_near(piece, 1).start()

    def column_done(self, k):
        for piece in self.columns[k]:
            which = self.pieces[piece][0]

            @pl.when(self.r != which)
            def _():
                for slot in range(2):
                    self.to_near(piece, slot).wait_recv()
                for slot in range(2):
                    self.to_near(piece, slot).wait_send()
                self.to_far(piece).wait_send()

                @pl.when(self.r + 2 < self.n_rows)
                def _():
                    self.to_row(piece, 0, self.r + 2, False).wait_send()

            @pl.when(self.r == which)
            def _():
                self.to_row(piece, 0, 1 - which, True).wait_send()
                if which + 2 < self.n_rows:
                    self.to_row(piece, 1, which + 2, True).wait_send()

    def part(self, ref, m):
        start = pl.multiple_of(self.c * self.share + m * self.chunk, 8)
        return ref.at[pl.ds(start, self.chunk), :]

    def gather(self, kind, s, m):
        q, p = self.q, self.p
        if kind == "dn":
            origin, dest, send, recv = q + s - 1, self.r - 2, self.dn_send, self.dn_recv
        else:
            origin, dest, send, recv = q - s + 1, self.r + 2, self.up_send, self.up_recv
        spot = self.gathered[m].at[2 * origin + p]
        src = self.part(self.panel, m) if s == 1 else spot
        return self.remote(src, spot, send.at[s - 1, m], recv.at[s - 1, m], dest, self.c)

    def awaited(self, kind, s, m):
        recv = self.dn_recv if kind == "dn" else self.up_recv
        send = self.dn_send if kind == "dn" else self.up_send
        row = self.r + 2 * s if kind == "dn" else self.r - 2 * s
        spot = self.gathered[m].at[row]
        return self.remote(spot, spot, send.at[s - 1, m], recv.at[s - 1, m], self.r, self.c)

    def across(self, origin, m, own):
        spot = self.gathered[m].at[2 * origin + self.p]
        src = self.part(self.panel, m) if own else spot
        return self.remote(src, spot, self.x_send.at[origin, m], self.x_recv.at[origin, m],
                           self.partner, self.c)

    def crossed(self, origin, m):
        spot = self.gathered[m].at[2 * origin + 1 - self.p]
        return self.remote(spot, spot, self.x_send.at[origin, m], self.x_recv.at[origin, m],
                           self.r, self.c)

    def open_down(self):
        @pl.when(self.q >= 1)
        def _():
            for m in range(CHUNKS):
                self.gather("dn", 1, m).start()
                self.across(self.q, m, True).start()

    def open_up(self):
        @pl.when((self.q >= 1) & (self.q + 1 < self.n_pos))
        def _():
            for m in range(CHUNKS):
                self.gather("up", 1, m).start()

    def round_down(self, s, m):
        if s < 1 or s > self.n_pos - 1:
            return

        @pl.when(self.q + s < self.n_pos)
        def _():
            self.awaited("dn", s, m).wait_recv()
            self.across(self.q + s, m, False).start()

            @pl.when(self.q >= 1)
            def _():
                self.gather("dn", s + 1, m).start()

    def round_up(self, s, m):
        if s < 1 or s > self.n_pos - 2:
            return

        @pl.when(self.q - s >= 1)
        def _():
            self.awaited("up", s, m).wait_recv()
            self.across(self.q - s, m, False).start()

            @pl.when(self.q + 1 < self.n_pos)
            def _():
                self.gather("up", s + 1, m).start()

    def keep_own(self):
        for m in range(CHUNKS):
            start = pl.multiple_of(self.c * self.share + m * self.chunk, 8)
            self.gathered[m][self.r] = self.own[pl.ds(start, self.chunk), :]

    def select(self, m, rows, live):
        for origin in range(1, self.n_pos):
            self.crossed(origin, m).wait_recv()
        start = pl.multiple_of(self.c * self.share + m * self.chunk, 8)
        for t in range(self.n_cols):
            value = self.gathered[m][rows[t]] * live[rows[t]].astype(jnp.float32)
            self.staged[m][t] = value

            @pl.when(self.c == t)
            def _():
                self.target[pl.ds(start, self.chunk), :] = value

    def deal(self, t, m):
        return self.remote(self.staged[m].at[t], self.part(self.target, m),
                           self.t_send.at[t, m], self.t_recv.at[self.c, m], self.r, t)

    def deal_all(self, m):
        for t in range(self.n_cols):

            @pl.when(self.c != t)
            def _():
                self.deal(t, m).start()

    def dealt(self, m):
        for i in range(1, self.n_cols):
            src = lax.rem(self.c + i, self.n_cols)
            start = pl.multiple_of(src * self.share + m * self.chunk, 8)
            spot = self.target.at[pl.ds(start, self.chunk), :]
            self.remote(spot, spot, self.t_send.at[src, m], self.t_recv.at[src, m], self.r, src).wait_recv()

    def finish(self):
        for m in range(CHUNKS):
            self.dealt(m)
            for t in range(self.n_cols):

                @pl.when(self.c != t)
                def _():
                    self.deal(t, m).wait_send()

            for s in range(1, self.n_pos):

                @pl.when((self.q >= 1) & (self.q + s - 1 < self.n_pos))
                def _():
                    self.gather("dn", s, m).wait_send()

                @pl.when((self.q + 1 < self.n_pos) & (self.q - s + 1 >= 1))
                def _():
                    self.gather("up", s, m).wait_send()

            for origin in range(1, self.n_pos):
                self.across(origin, m, False).wait_send()


def window_kernel(n_rows, n_cols, window_rows, row_live, panel, factor, solved, target,
                  own, lower, inverses, aug, upper, leaf_inv, *rest):
    gathered, staged = rest[:CHUNKS], rest[CHUNKS : 2 * CHUNKS]
    own_sem, sems = rest[2 * CHUNKS], rest[2 * CHUNKS + 1 :]
    net = Traffic(n_rows, n_cols, panel, own, lower, target, gathered, staged, sems)
    width = panel.shape[0]
    total = lower.shape[0]
    n_leaf = total // LEAF
    n_pos = n_rows // 2
    r = lax.axis_index("rows")
    fetch = pltpu.make_async_copy(panel, own, own_sem)
    fetch.start()
    net.barrier()
    net.send_diagonal()
    net.open_down()
    rows = lax.broadcasted_iota(jnp.int32, (LEAF, LEAF), 0)
    lanes = lax.broadcasted_iota(jnp.int32, (LEAF, LEAF), 1)
    inverses[...] = jnp.zeros(inverses.shape, jnp.float32)
    fetch.wait()

    @pl.when(r == 0)
    def _():
        lower[:width, :width] = own[:, :width]

    @pl.when(r == 1)
    def _():
        lower[width:, :] = own[...]

    for b in range(n_leaf - 1):
        lower[b * LEAF : (b + 1) * LEAF, (b + 1) * LEAF :] = jnp.zeros(
            (LEAF, total - (b + 1) * LEAF), jnp.float32)
    net.keep_own()
    net.column_in(0)
    net.column_in(1)
    net.column_far(0)
    net.column_far(1)
    net.column_in(2)
    net.column_done(0)
    net.open_up()
    for m in range(CHUNKS):
        for s in range(1, n_pos - 2):
            net.round_down(s, m)
            net.round_up(s - 1, m)

    def before(b):
        if b + 3 < n_leaf:
            net.column_in(b + 3)
        if b + 1 < n_leaf:
            net.column_done(b + 1)

    def after(b):
        if b + 2 < n_leaf:
            net.column_far(b + 2)
        half = [(0, 1), (2, 3)]
        if b in (1, 2):
            for m in half[b - 1]:
                net.round_down(n_pos - 2, m)
                net.round_up(n_pos - 3, m)
        if b in (3, 4):
            for m in half[b - 3]:
                net.round_down(n_pos - 1, m)
                net.round_up(n_pos - 2, m)

    def step(k, carry):
        at = pl.ds(pl.multiple_of(k * LEAF, LEAF), LEAF)
        block = lower[at, at]
        aug[:, :LEAF] = jnp.where(rows >= lanes, block, block.T)
        aug[:, LEAF:] = jnp.where(rows == lanes, 1.0, 0.0)
        factor_leaf(aug, upper, leaf_inv)
        lower[at, at] = upper[...].T
        for b in range(n_leaf):

            @pl.when(k == b)
            def _():
                before(b)
                if b in (5, 6):
                    for m in ((0, 1), (2, 3))[b - 5]:
                        net.select(m, window_rows, row_live)
                lo, hi = b * LEAF, (b + 1) * LEAF
                wide = b * LEAF // WIDE
                off = lo - wide * WIDE
                inv = leaf_inv[...]
                inverses[wide, off : off + LEAF, off : off + LEAF] = inv
                if off:
                    early = inverses[wide, :LEAF, :LEAF]
                    cross = lower[lo:hi, lo - LEAF : lo]
                    part = lax.dot_general(
                        cross, early, (((1,), (0,)), ((), ())), precision=HIGHEST,
                        preferred_element_type=jnp.float32)
                    inverses[wide, LEAF:, :LEAF] = -lax.dot_general(
                        inv, part, (((1,), (0,)), ((), ())), precision=HIGHEST,
                        preferred_element_type=jnp.float32)
                if hi < total:
                    lower[hi:, lo:hi] = times_trans(lower[hi:, lo:hi], inv)
                    nxt = hi + LEAF
                    lower[hi:, hi:nxt] = lower[hi:, hi:nxt] - times_trans(
                        lower[hi:, :hi], lower[hi:nxt, :hi])
                if b in (5, 6):
                    for m in ((0, 1), (2, 3))[b - 5]:
                        net.deal_all(m)
                after(b)

        return carry

    lax.fori_loop(0, n_leaf, step, 0)

    n_wide = total // WIDE
    live = jnp.where(r < P_SIZE, 1, row_live[r]).astype(jnp.float32)

    @pl.when(r < P_SIZE)
    def _():
        factor[...] = lower[pl.ds(pl.multiple_of(lax.rem(r, P_SIZE) * width, width), width), :]

    @pl.when(r >= P_SIZE)
    def _():
        factor[...] = own[...] * live
        for wide in range(n_wide):
            lo, hi = wide * WIDE, (wide + 1) * WIDE
            now = factor[:, lo:hi]
            if wide:
                now = now - times_trans(factor[:, :lo], lower[lo:hi, :lo])
            factor[:, lo:hi] = times_trans(now, inverses[wide])

    for wide in reversed(range(n_wide)):
        lo, hi = wide * WIDE, (wide + 1) * WIDE
        now = factor[:, lo:hi]
        if hi < total:
            now = now - times(solved[:, hi:], lower[hi:, lo:hi])
        solved[:, lo:hi] = times(now, inverses[wide])
    net.finish()


def factor_window(window_rows, row_live, panel, n_rows, n_cols):
    if n_cols != 4 or n_rows < 4 or n_rows % 2:
        raise ValueError("unsupported mesh")
    width, total = panel.shape
    n_leaf = total // LEAF
    n_pieces = n_leaf + width // LEAF
    n_pos = n_rows // 2
    chunk = width // n_cols // CHUNKS
    dma = pltpu.SemaphoreType.DMA
    return pl.pallas_call(
        functools.partial(window_kernel, n_rows, n_cols),
        out_shape=(jax.ShapeDtypeStruct(panel.shape, jnp.float32),) * 3,
        in_specs=[pl.BlockSpec(memory_space=pltpu.SMEM)] * 2 + [pl.BlockSpec(memory_space=pltpu.HBM)],
        out_specs=(pl.BlockSpec(memory_space=pltpu.VMEM),) * 3,
        scratch_shapes=[
            pltpu.VMEM(panel.shape, jnp.float32),
            pltpu.VMEM((total, total), jnp.float32),
            pltpu.VMEM((total // WIDE, WIDE, WIDE), jnp.float32),
            pltpu.VMEM((LEAF, 2 * LEAF), jnp.float32),
            pltpu.VMEM((LEAF, LEAF), jnp.float32),
            pltpu.VMEM((LEAF, LEAF), jnp.float32),
        ] + [pltpu.VMEM((n_rows, chunk, total), jnp.float32)] * CHUNKS
        + [pltpu.VMEM((n_cols, chunk, total), jnp.float32)] * CHUNKS
        + [
            dma(()),
            dma((n_pieces, 2)), dma((n_pieces,)), dma((n_pieces,)), dma((n_pieces,)),
            dma((n_pieces, 2)), dma((n_pieces, 2)),
            dma((n_pos, CHUNKS)), dma((n_pos, CHUNKS)), dma((n_pos, CHUNKS)), dma((n_pos, CHUNKS)),
            dma((n_pos, CHUNKS)), dma((n_pos, CHUNKS)),
            dma((n_cols, CHUNKS)), dma((n_cols, CHUNKS)),
        ],
        compiler_params=pltpu.CompilerParams(
            collective_id=0, has_side_effects=True, vmem_limit_bytes=(32 << 20) + n_rows * width * total * 4 // n_cols),
        cost_estimate=pl.CostEstimate(flops=10**10, bytes_accessed=10**7, transcendentals=0),
        name="factor_window",
    )(window_rows, row_live, panel)


def update_kernel(factor, solved, target, window, factor_out, updated, sem):
    store = pltpu.make_async_copy(factor, factor_out, sem)
    store.start()
    updated[...] = window[...] - times_trans(solved[...], target[...])
    store.wait()


def update_window(factor, solved, target, window):
    return pl.pallas_call(
        update_kernel,
        out_shape=(jax.ShapeDtypeStruct(factor.shape, jnp.float32),
                   jax.ShapeDtypeStruct(window.shape, jnp.float32)),
        in_specs=[pl.BlockSpec(memory_space=pltpu.VMEM)] * 4,
        out_specs=(pl.BlockSpec(memory_space=pltpu.HBM), pl.BlockSpec(memory_space=pltpu.VMEM)),
        scratch_shapes=[pltpu.SemaphoreType.DMA(())],
        compiler_params=pltpu.CompilerParams(vmem_limit_bytes=40 << 20),
        cost_estimate=pl.CostEstimate(flops=10**9, bytes_accessed=10**7, transcendentals=0),
        name="update_window",
    )(factor, solved, target, window)


def shards(n_rows, n_cols, panel, window_block, row_live, window_rows):
    factor, solved, target = factor_window(window_rows, row_live, panel, n_rows, n_cols)
    return update_window(factor, solved, target, window_block)


def solution(mesh):
    in_specs = (P("rows", None), P("rows", "cols"), P(), P())
    out_specs = (P("rows", None), P("rows", "cols"))
    body = functools.partial(shards, mesh.shape["rows"], mesh.shape["cols"])
    return jax.shard_map(body, mesh=mesh, in_specs=in_specs, out_specs=out_specs, check_vma=False)
```

```python
import functools

import jax
import jax.numpy as jnp
from jax import lax
from jax.experimental import pallas as pl
from jax.experimental.pallas import tpu as pltpu
from jax.sharding import PartitionSpec as P

P_SIZE = 2
CONTRACT = (((1,), (1,)), ((), ()))
LEAF = 128
GROUP = 16
CHUNKS = 4
MESH = pl.DeviceIdType.MESH


def halves(value):
    high = value.astype(jnp.bfloat16)
    return high, (value - high.astype(jnp.float32)).astype(jnp.bfloat16)


def product(left, right, contract):
    lh, ll = halves(left)
    rh, rl = halves(right)

    def dot(a, b):
        return lax.dot_general(a, b, contract, preferred_element_type=jnp.float32)

    return dot(lh, rh) + (dot(lh, rl) + dot(ll, rh))


def times_trans(left, right):
    return product(left, right, CONTRACT)


def split3(value):
    high = value.astype(jnp.bfloat16).astype(jnp.float32)
    rest = value - high
    mid = rest.astype(jnp.bfloat16).astype(jnp.float32)
    return high, mid, rest - mid


def factor_leaf(aug, upper, inverse):
    lanes = lax.broadcasted_iota(jnp.int32, (GROUP, LEAF), 1)
    subs = lax.broadcasted_iota(jnp.int32, (GROUP, LEAF), 0)
    for g in range(LEAF // GROUP):
        base = g * GROUP
        left = aug[base : base + GROUP, :LEAF]
        right = aug[base : base + GROUP, LEAF:]
        cols = [
            jnp.broadcast_to(left[:, base + j : base + j + 1], (GROUP, LEAF)) for j in range(GROUP)
        ]
        scale = jnp.zeros((GROUP, LEAF), jnp.float32)
        for k in range(GROUP):
            pivot = jnp.broadcast_to(cols[k][k : k + 1, :], (GROUP, LEAF))
            root = lax.rsqrt(pivot)
            scale = jnp.where(subs == k, root, scale)
            if k + 1 < GROUP:
                mult = jnp.where(subs > k, cols[k] * (root * root), 0.0)
                for j in range(k + 1, GROUP):
                    cols[j] = cols[j] - mult * jnp.broadcast_to(cols[j][k : k + 1, :], (GROUP, LEAF))
                left = left - mult * jnp.broadcast_to(left[k : k + 1, :], (GROUP, LEAF))
                right = right - mult * jnp.broadcast_to(right[k : k + 1, :], (GROUP, LEAF))
        row_of = lanes - base
        left = jnp.where(row_of >= subs, left * scale, 0.0)
        right = right * scale
        upper[base : base + GROUP, :] = left
        inverse[base : base + GROUP, :] = right
        if base + GROUP < LEAF:
            lh, lm, ll = split3(left)
            rh, rm, rl = split3(right)
            keep = lanes >= base + GROUP
            a = [jnp.where(keep, v, 0.0) for v in (lh, lm, ll)]
            lhs = jnp.concatenate([a[0], a[0], a[1], a[0], a[1], a[2]], axis=0)
            rl_ = jnp.concatenate([lh, lm, lh, ll, lm, lh], axis=0)
            rr_ = jnp.concatenate([rh, rm, rh, rl, rm, rh], axis=0)
            rhs = jnp.concatenate([rl_, rr_], axis=1)
            update = lax.dot_general(
                lhs, rhs, (((0,), (0,)), ((), ())), preferred_element_type=jnp.float32)
            aug[base + GROUP :, :] = aug[base + GROUP :, :] - update[base + GROUP :, :]


def remote(src, dst, send, recv, row, col):
    return pltpu.make_async_remote_copy(
        src_ref=src, dst_ref=dst, send_sem=send, recv_sem=recv,
        device_id=(row, col), device_id_type=MESH)


class Place:
    def __init__(self, n_rows, n_cols):
        self.n_rows, self.n_cols = n_rows, n_cols
        self.n_pos = n_rows // 2
        self.r = lax.axis_index("rows")
        self.c = lax.axis_index("cols")
        self.q = lax.div(self.r, 2)
        self.p = lax.rem(self.r, 2)
        self.partner = self.r + 1 - 2 * self.p
        self.far = lax.rem(self.c + 2, 4)
        self.near = self.c + 1 - 2 * lax.rem(self.c, 2)
        self.leads = self.q == 0
        self.follows = self.q >= 1
        self.passes = self.q + 1 < self.n_pos

    def barrier(self):
        sem = pltpu.get_barrier_semaphore()

        def greet(row, col):
            pl.semaphore_signal(sem, inc=1, device_id=(row, col), device_id_type=MESH)

        for i in range(1, self.n_cols):
            greet(self.r, lax.rem(self.c + i, self.n_cols))
        greet(self.partner, self.c)

        @pl.when(self.leads)
        def _():
            for s in range(1, self.n_pos):
                greet(self.r + 2 * s, self.c)
            pl.semaphore_wait(sem, self.n_cols + self.n_pos - 1)

        @pl.when(self.follows)
        def _():
            greet(self.p, self.c)

            @pl.when(self.q >= 2)
            def _():
                greet(self.r - 2, self.c)

            @pl.when(self.passes)
            def _():
                greet(self.r + 2, self.c)

            extra = (self.q >= 2).astype(jnp.int32) + self.passes.astype(jnp.int32)
            pl.semaphore_wait(sem, self.n_cols + 1 + extra)


class Blocks:
    def __init__(self, at, lower, pieces, sems):
        self.at, self.lower, self.pieces = at, lower, pieces
        (self.row_send, self.row_recv, self.far_send, self.far_recv, self.near_send, self.near_recv) = sems

    def of(self, k):
        return [i for i, piece in enumerate(self.pieces) if piece[3] == k]

    def place(self, piece, owner, ref=None, base=0):
        _, lo, size, k = self.pieces[piece]
        start = pl.multiple_of(lo - base + owner * (size // 4), 8)
        spot = (pl.ds(start, size // 4), pl.ds(k * LEAF, LEAF))
        return (self.lower if ref is None else ref).at[spot]

    def to_row(self, piece, slot, src=None):
        at = self.at
        spot = self.place(piece, at.c)
        return remote(spot if src is None else src, spot, self.row_send.at[piece, slot],
                      self.row_recv.at[piece], (at.r + 2, at.partner)[slot], at.c)

    def to_far(self, piece):
        at = self.at
        spot = self.place(piece, at.c)
        return remote(spot, spot, self.far_send.at[piece], self.far_recv.at[piece], at.r, at.far)

    def to_near(self, piece, slot):
        at = self.at
        spot = self.place(piece, (at.c, at.far)[slot])
        return remote(spot, spot, self.near_send.at[piece, slot], self.near_recv.at[piece, slot], at.r, at.near)

    def share(self, piece):
        self.to_far(piece).start()
        self.to_near(piece, 0).start()

    def share_far(self, piece):
        self.to_far(piece).wait_recv()
        self.to_near(piece, 1).start()

    def shared(self, piece):
        for slot in range(2):
            self.to_near(piece, slot).wait_recv()
        for slot in range(2):
            self.to_near(piece, slot).wait_send()
        self.to_far(piece).wait_send()


class Raw(Blocks):
    def send(self, panel, width):
        for piece, (which, _, _, _) in enumerate(self.pieces):

            @pl.when(self.at.r == which)
            def _():
                self.to_row(piece, 1, self.place(piece, self.at.c, panel, which * width)).start()

    def column(self, k, stage):
        for piece in self.of(k):
            which = self.pieces[piece][0]

            @pl.when(self.at.p != which)
            def _():
                if stage == 0:
                    self.to_row(piece, 1).wait_recv()
                    self.share(piece)
                elif stage == 1:
                    self.share_far(piece)
                else:
                    self.shared(piece)

            if stage == 2:

                @pl.when(self.at.p == which)
                def _():
                    self.to_row(piece, 1).wait_send()


class Solved(Blocks):
    def send(self, k):
        for piece in self.of(k):

            @pl.when(self.at.p == self.pieces[piece][0])
            def _():
                self.to_row(piece, 0).start()

    def sent(self, k):
        for piece in self.of(k):

            @pl.when(self.at.p == self.pieces[piece][0])
            def _():
                self.to_row(piece, 0).wait_send()

    def take(self, k):
        at = self.at
        for piece in self.of(k):

            @pl.when(at.p == self.pieces[piece][0])
            def _():
                self.to_row(piece, 0).wait_recv()

                @pl.when(at.passes)
                def _():
                    self.to_row(piece, 0).start()

                self.to_row(piece, 1).start()
                self.share(piece)

        for piece in self.of(k):

            @pl.when(at.p != self.pieces[piece][0])
            def _():
                self.to_row(piece, 1).wait_recv()
                self.share(piece)

    def take_far(self, k):
        for piece in self.of(k):
            self.share_far(piece)

    def taken(self, k):
        at = self.at
        for piece in self.of(k):
            self.shared(piece)

            @pl.when(at.p == self.pieces[piece][0])
            def _():
                self.to_row(piece, 1).wait_send()

                @pl.when(at.passes)
                def _():
                    self.to_row(piece, 0).wait_send()


class Rows:
    def __init__(self, at, panel, own, target, gathered, staged, sems):
        self.at, self.panel, self.own, self.target = at, panel, own, target
        self.gathered, self.staged = gathered, staged
        (self.dn_send, self.dn_recv, self.up_send, self.up_recv, self.x_send, self.x_recv,
         self.t_send, self.t_recv, self.l_send, self.l_recv) = sems
        self.width = panel.shape[0]
        self.share = self.width // at.n_cols
        self.chunk = self.share // CHUNKS

    def part(self, ref, m, owner=None):
        owner = self.at.c if owner is None else owner
        start = pl.multiple_of(owner * self.share + m * self.chunk, 8)
        return ref.at[pl.ds(start, self.chunk), :]

    def chain(self, kind, s, m):
        at = self.at
        if kind == "dn":
            origin, dest, send, recv = at.r + 2 * (s - 1), at.r - 2, self.dn_send, self.dn_recv
        else:
            origin, dest, send, recv = at.r - 2 * (s - 1), at.r + 2, self.up_send, self.up_recv
        spot = self.gathered[m].at[origin]
        src = self.part(self.panel, m) if s == 1 else spot
        return remote(src, spot, send.at[s - 1, m], recv.at[s - 1, m], dest, at.c)

    def awaited(self, kind, s, m):
        at = self.at
        recv, send = (self.dn_recv, self.dn_send) if kind == "dn" else (self.up_recv, self.up_send)
        spot = self.gathered[m].at[at.r + 2 * s if kind == "dn" else at.r - 2 * s]
        return remote(spot, spot, send.at[s - 1, m], recv.at[s - 1, m], at.r, at.c)

    def across(self, origin, m, own):
        at = self.at
        spot = self.gathered[m].at[2 * origin + at.p]
        src = self.part(self.panel, m) if own else spot
        return remote(src, spot, self.x_send.at[origin, m], self.x_recv.at[origin, m], at.partner, at.c)

    def crossed(self, origin, m):
        at = self.at
        spot = self.gathered[m].at[2 * origin + 1 - at.p]
        return remote(spot, spot, self.x_send.at[origin, m], self.x_recv.at[origin, m], at.r, at.c)

    def open(self):
        at = self.at
        for m in range(CHUNKS):

            @pl.when(at.q >= 2)
            def _():
                self.chain("dn", 1, m).start()

            @pl.when(at.passes)
            def _():
                self.chain("up", 1, m).start()

            self.across(at.q, m, True).start()

    def keep_own(self):
        for m in range(CHUNKS):
            start = pl.multiple_of(self.at.c * self.share + m * self.chunk, 8)
            self.gathered[m][self.at.r] = self.own[pl.ds(start, self.chunk), :]

    def relay(self, s, m):
        at = self.at

        @pl.when(at.q + s < at.n_pos)
        def _():
            self.awaited("dn", s, m).wait_recv()
            self.across(at.q + s, m, False).start()

            @pl.when(at.q >= 2)
            def _():
                self.chain("dn", s + 1, m).start()

        @pl.when(at.q - s >= 1)
        def _():
            self.awaited("up", s, m).wait_recv()
            self.across(at.q - s, m, False).start()

            @pl.when(at.passes)
            def _():
                self.chain("up", s + 1, m).start()

    def select(self, m, rows, live):
        at = self.at
        for origin in range(1, at.n_pos):
            self.crossed(origin, m).wait_recv()
        start = pl.multiple_of(at.c * self.share + m * self.chunk, 8)
        for t in range(at.n_cols):
            value = self.gathered[m][rows[t]] * live[rows[t]].astype(jnp.float32)
            self.staged[m][t] = value

            @pl.when(at.c == t)
            def _():
                self.target[pl.ds(start, self.chunk), :] = value

    def deal(self, t, m):
        at = self.at
        return remote(self.staged[m].at[t], self.part(self.target, m), self.t_send.at[t, m],
                      self.t_recv.at[at.c, m], at.r, t)

    def deal_all(self, m):
        for t in range(self.at.n_cols):

            @pl.when(self.at.c != t)
            def _():
                self.deal(t, m).start()

    def to_leader(self, owner, m):
        at = self.at
        start = pl.multiple_of(owner * self.share + m * self.chunk, 8)
        rows = pl.ds(start, self.chunk)
        src = self.target.at[rows, pl.ds(pl.multiple_of(at.p * self.width, LEAF), self.width)]
        return remote(src, self.target.at[rows, pl.ds(0, self.width)], self.l_send.at[owner, m],
                      self.l_recv.at[owner, m], at.p, at.c)

    def dealt(self, m):
        at = self.at
        for i in range(1, at.n_cols):
            src = lax.rem(at.c + i, at.n_cols)
            spot = self.part(self.target, m, src)
            remote(spot, spot, self.t_send.at[src, m], self.t_recv.at[src, m], at.r, src).wait_recv()

        @pl.when(at.q == 1)
        def _():
            for owner in range(at.n_cols):
                self.to_leader(owner, m).start()

    def arrived(self):
        for m in range(CHUNKS):
            for owner in range(self.at.n_cols):
                self.to_leader(owner, m).wait_recv()

    def finish(self):
        at = self.at
        for m in range(CHUNKS):
            for t in range(at.n_cols):

                @pl.when(at.c != t)
                def _():
                    self.deal(t, m).wait_send()

                @pl.when(at.q == 1)
                def _():
                    self.to_leader(t, m).wait_send()

            for s in range(1, at.n_pos - 1):

                @pl.when((at.q >= 2) & (at.q + s - 1 < at.n_pos))
                def _():
                    self.chain("dn", s, m).wait_send()

                @pl.when(at.passes & (at.q - s + 1 >= 1))
                def _():
                    self.chain("up", s, m).wait_send()

            for origin in range(1, at.n_pos):
                self.across(origin, m, False).wait_send()


def lead(at, raw, solved, send_inverse, own, lower, inverses, aug, upper):
    width = own.shape[0]
    total = lower.shape[0]
    n_leaf = total // LEAF
    rows = lax.broadcasted_iota(jnp.int32, (LEAF, LEAF), 0)
    lanes = lax.broadcasted_iota(jnp.int32, (LEAF, LEAF), 1)

    @pl.when(at.r == 0)
    def _():
        lower[:width, :width] = own[:, :width]

    @pl.when(at.r == 1)
    def _():
        lower[width:, :] = own[...]

    for b in range(n_leaf - 1):
        lower[b * LEAF : (b + 1) * LEAF, (b + 1) * LEAF :] = jnp.zeros(
            (LEAF, total - (b + 1) * LEAF), jnp.float32)
    raw.column(0, 0)
    raw.column(1, 0)
    raw.column(0, 1)
    raw.column(2, 0)
    raw.column(1, 1)
    raw.column(0, 2)

    def step(k, carry):
        here = pl.ds(pl.multiple_of(k * LEAF, LEAF), LEAF)
        block = lower[here, here]
        aug[:, :LEAF] = jnp.where(rows >= lanes, block, block.T)
        aug[:, LEAF:] = jnp.where(rows == lanes, 1.0, 0.0)
        factor_leaf(aug, upper, inverses.at[k])
        lower[here, here] = upper[...].T
        for b in range(n_leaf):

            @pl.when(k == b)
            def _():
                if b + 3 < n_leaf:
                    raw.column(b + 3, 0)
                if b + 2 < n_leaf:
                    raw.column(b + 2, 1)
                if b + 1 < n_leaf:
                    raw.column(b + 1, 2)
                lo, hi = b * LEAF, (b + 1) * LEAF
                send_inverse(b)
                if hi < total:
                    lower[hi:, lo:hi] = times_trans(lower[hi:, lo:hi], inverses[b])
                    nxt = hi + LEAF
                    lower[hi:, hi:nxt] = lower[hi:, hi:nxt] - times_trans(
                        lower[hi:, :hi], lower[hi:nxt, :hi])
                    solved.send(b)

        return carry

    lax.fori_loop(0, n_leaf, step, 0)


def window_kernel(n_rows, n_cols, rows_in, live_in, panel, window, factor, other, updated,
                  window_rows, row_live, own, lower, target, inverses, aug, upper, *rest):
    gathered, staged = rest[:CHUNKS], rest[CHUNKS : 2 * CHUNKS]
    own_sem, window_sem, rows_sem, live_sem = rest[2 * CHUNKS : 2 * CHUNKS + 4]
    sems = rest[2 * CHUNKS + 4 :]
    inv_send, inv_recv = sems[:2]
    at = Place(n_rows, n_cols)
    width = panel.shape[0]
    total = lower.shape[0]
    n_leaf = total // LEAF
    per = width // LEAF
    raw_pieces = [
        (which, which * width + max(0, k - which * per) * LEAF, width - max(0, k - which * per) * LEAF, k)
        for k in range(n_leaf) for which in range(2) if k < (which + 1) * per
    ]
    low_pieces = [
        (half, (k + 1) * LEAF + half * (total - (k + 1) * LEAF) // 2, (total - (k + 1) * LEAF) // 2, k)
        for k in range(n_leaf - 1) for half in range(2)
    ]
    raw = Raw(at, lower, raw_pieces, sems[2:8])
    solved = Solved(at, lower, low_pieces, sems[8:14])
    net = Rows(at, panel, own, target, gathered, staged, sems[14:])
    fetches = [
        pltpu.make_async_copy(panel, own, own_sem),
        pltpu.make_async_copy(window, updated, window_sem),
        pltpu.make_async_copy(rows_in, window_rows, rows_sem),
        pltpu.make_async_copy(live_in, row_live, live_sem),
    ]
    for fetch in fetches:
        fetch.start()
    at.barrier()

    def inverse(b, s):
        spot = inverses.at[b]
        return remote(spot, spot, inv_send.at[b, s - 1], inv_recv.at[b], at.r + 2 * s, at.c)

    def send_inverse(b):
        for s in reversed(range(1, at.n_pos)):
            inverse(b, s).start()

    @pl.when(at.leads)
    def _():
        raw.send(panel, width)

    @pl.when(at.follows)
    def _():
        net.open()

    for fetch in fetches:
        fetch.wait()
    live = row_live[at.r].astype(jnp.float32)

    @pl.when(at.leads)
    def _():
        lead(at, raw, solved, send_inverse, own, lower, inverses, aug, upper)
        factor[...] = lower[pl.ds(pl.multiple_of(at.p * width, width), width), :]
        for b in range(n_leaf):
            for s in range(1, at.n_pos):
                inverse(b, s).wait_send()
        for b in range(n_leaf - 1):
            solved.sent(b)
        net.arrived()
        updated[...] = updated[...] - target[:, :width].T

    @pl.when(at.follows)
    def _():
        net.keep_own()

        def ready(src, dst, b, scale):
            lo, hi = b * LEAF, (b + 1) * LEAF
            now = src[:, lo:hi]
            if scale is not None:
                now = now * scale
            if b:
                now = now - times_trans(dst[:, :lo], lower[lo:hi, :lo])
            dst[:, lo:hi] = now

        def close(dst, b):
            lo, hi = b * LEAF, (b + 1) * LEAF
            dst[:, lo:hi] = times_trans(dst[:, lo:hi], inverses[b])

        for b in range(n_leaf):
            if b == 1:
                for s in range(1, at.n_pos - 2):
                    for m in range(CHUNKS):
                        net.relay(s, m)
            if b in (2, 3) and at.n_pos > 2:
                for m in ((0, 1), (2, 3))[b - 2]:
                    net.relay(at.n_pos - 2, m)
            if 3 <= b < 3 + CHUNKS:
                net.select(b - 3, window_rows, row_live)
            if b:
                solved.take(b - 1)
                solved.take_far(b - 1)
            if 3 <= b < 3 + CHUNKS:
                net.deal_all(b - 3)
            if 5 <= b < 5 + CHUNKS:
                net.dealt(b - 5)
            if b:
                solved.taken(b - 1)
            ready(own, factor, b, live)
            if b == n_leaf - 1:
                net.dealt(CHUNKS - 1)
                for k in range(b):
                    ready(target, other, k, None)
                    close(other, k)
                ready(target, other, b, None)
                lo = b * LEAF
                updated[...] = updated[...] - times_trans(factor[:, :lo], other[:, :lo])
            inverse(b, 0).wait_recv()
            close(factor, b)
        close(other, n_leaf - 1)
        net.finish()


def factor_window(window_rows, row_live, panel, window, n_rows, n_cols):
    if n_cols != 4 or n_rows < 6 or n_rows % 2:
        raise ValueError("unsupported mesh")
    width, total = panel.shape
    n_leaf = total // LEAF
    n_raw = n_leaf + width // LEAF
    n_low = 2 * (n_leaf - 1)
    n_pos = n_rows // 2
    chunk = width // n_cols // CHUNKS
    dma = pltpu.SemaphoreType.DMA
    tall = jax.ShapeDtypeStruct(panel.shape, jnp.float32)
    return pl.pallas_call(
        functools.partial(window_kernel, n_rows, n_cols),
        out_shape=(tall, tall, jax.ShapeDtypeStruct(window.shape, jnp.float32)),
        in_specs=[pl.BlockSpec(memory_space=pltpu.HBM)] * 4,
        out_specs=(pl.BlockSpec(memory_space=pltpu.VMEM),) * 3,
        scratch_shapes=[
            pltpu.SMEM(window_rows.shape, jnp.int32),
            pltpu.SMEM(row_live.shape, jnp.int32),
            pltpu.VMEM(panel.shape, jnp.float32),
            pltpu.VMEM((total, total), jnp.float32),
            pltpu.VMEM(panel.shape, jnp.float32),
            pltpu.VMEM((n_leaf, LEAF, LEAF), jnp.float32),
            pltpu.VMEM((LEAF, 2 * LEAF), jnp.float32),
            pltpu.VMEM((LEAF, LEAF), jnp.float32),
        ] + [pltpu.VMEM((n_rows, chunk, total), jnp.float32)] * CHUNKS
        + [pltpu.VMEM((n_cols, chunk, total), jnp.float32)] * CHUNKS
        + [
            dma(()), dma(()), dma(()), dma(()),
            dma((n_leaf, n_pos - 1)), dma((n_leaf,)),
            dma((n_raw, 2)), dma((n_raw,)), dma((n_raw,)), dma((n_raw,)), dma((n_raw, 2)), dma((n_raw, 2)),
            dma((n_low, 2)), dma((n_low,)), dma((n_low,)), dma((n_low,)), dma((n_low, 2)), dma((n_low, 2)),
            dma((n_pos, CHUNKS)), dma((n_pos, CHUNKS)), dma((n_pos, CHUNKS)), dma((n_pos, CHUNKS)),
            dma((n_pos, CHUNKS)), dma((n_pos, CHUNKS)),
            dma((n_cols, CHUNKS)), dma((n_cols, CHUNKS)), dma((n_cols, CHUNKS)), dma((n_cols, CHUNKS)),
        ],
        compiler_params=pltpu.CompilerParams(
            collective_id=0, has_side_effects=True, vmem_limit_bytes=(21 << 20) + n_rows * n_cols * CHUNKS * chunk * total),
        cost_estimate=pl.CostEstimate(flops=10**10, bytes_accessed=10**7, transcendentals=0),
        name="factor_window",
    )(*[pltpu.with_memory_space_constraint(x, pltpu.HBM) for x in (window_rows, row_live, panel, window)])


def update_kernel(factor, other, partial, factor_out, updated, sem):
    store = pltpu.make_async_copy(factor, factor_out, sem)
    store.start()
    r = lax.axis_index("rows")
    lo = factor.shape[1] - LEAF

    @pl.when(r < P_SIZE)
    def _():
        updated[...] = partial[...]

    @pl.when(r >= P_SIZE)
    def _():
        updated[...] = partial[...] - times_trans(factor[:, lo:], other[:, lo:])

    store.wait()


def update_window(factor, other, partial):
    return pl.pallas_call(
        update_kernel,
        out_shape=(jax.ShapeDtypeStruct(factor.shape, jnp.float32),
                   jax.ShapeDtypeStruct(partial.shape, jnp.float32)),
        in_specs=[pl.BlockSpec(memory_space=pltpu.VMEM)] * 3,
        out_specs=(pl.BlockSpec(memory_space=pltpu.HBM), pl.BlockSpec(memory_space=pltpu.VMEM)),
        scratch_shapes=[pltpu.SemaphoreType.DMA(())],
        compiler_params=pltpu.CompilerParams(vmem_limit_bytes=24 << 20),
        cost_estimate=pl.CostEstimate(flops=10**9, bytes_accessed=10**7, transcendentals=0),
        name="update_window",
    )(factor, other, partial)


def shards(n_rows, n_cols, panel, window_block, row_live, window_rows):
    factor, other, partial = factor_window(window_rows, row_live, panel, window_block, n_rows, n_cols)
    return update_window(factor, other, partial)


def solution(mesh):
    in_specs = (P("rows", None), P("rows", "cols"), P(), P())
    out_specs = (P("rows", None), P("rows", "cols"))
    body = functools.partial(shards, mesh.shape["rows"], mesh.shape["cols"])
    return jax.shard_map(body, mesh=mesh, in_specs=in_specs, out_specs=out_specs, check_vma=False)
```

```python
import functools

import jax
import jax.numpy as jnp
from jax import lax
from jax.experimental import pallas as pl
from jax.experimental.pallas import tpu as pltpu
from jax.sharding import PartitionSpec as P

P_SIZE = 2
CONTRACT = (((1,), (1,)), ((), ()))
LEAF = 128
GROUP = 16
CHUNKS = 4
MESH = pl.DeviceIdType.MESH


def halves(value):
    high = value.astype(jnp.bfloat16)
    return high, (value - high.astype(jnp.float32)).astype(jnp.bfloat16)


def product(left, right):
    (lh, ll), (rh, rl) = left, right

    def dot(a, b):
        return lax.dot_general(a, b, CONTRACT, preferred_element_type=jnp.float32)

    return dot(lh, rh) + (dot(lh, rl) + dot(ll, rh))


def times_trans(left, right):
    return product(halves(left), halves(right))


class Split:
    def __init__(self, high, low):
        self.high, self.low = high, low

    def put(self, rows, cols, value):
        self.high[rows, cols], self.low[rows, cols] = halves(value)

    def get(self, rows, cols):
        return self.high[rows, cols], self.low[rows, cols]


def spread_row(value, k):
    return jnp.broadcast_to(value[k : k + 1, :], value.shape)


def factor_leaf(aug, upper, inverse):
    half = GROUP // 2
    subs = lax.broadcasted_iota(jnp.int32, (half, LEAF), 0)
    row_of = lax.broadcasted_iota(jnp.int32, (GROUP, LEAF), 1) - lax.broadcasted_iota(jnp.int32, (GROUP, LEAF), 0)
    lanes = lax.broadcasted_iota(jnp.int32, (GROUP, LEAF), 1)
    for g in range(LEAF // GROUP):
        base = g * GROUP
        parts = [[aug[base + h * half : base + (h + 1) * half, s * LEAF : (s + 1) * LEAF] for s in range(2)]
                 for h in range(2)]
        cols = [[jnp.broadcast_to(parts[h][0][:, base + j : base + j + 1], (half, LEAF)) for j in range(GROUP)]
                for h in range(2)]
        scales = [jnp.zeros((half, LEAF), jnp.float32)] * 2
        for k in range(GROUP):
            h, kk = k // half, k % half
            root = lax.rsqrt(spread_row(cols[h][k], kk))
            scales[h] = jnp.where(subs == kk, root, scales[h])
            if k + 1 == GROUP:
                break
            inv = root * root
            mults = {i: cols[i][k] * inv for i in range(h, 2)}
            for j in range(k + 1, GROUP):
                row = spread_row(cols[h][j], kk)
                for i in range(h, 2):
                    cols[i][j] = cols[i][j] - mults[i] * row
            mults[h] = jnp.where(subs > kk, mults[h], 0.0)
            for s in range(2):
                row = spread_row(parts[h][s], kk)
                for i in range(h, 2):
                    parts[i][s] = parts[i][s] - mults[i] * row
        left = jnp.concatenate([parts[h][0] * scales[h] for h in range(2)], axis=0)
        right = jnp.concatenate([parts[h][1] * scales[h] for h in range(2)], axis=0)
        left = jnp.where(row_of >= base, left, 0.0)
        upper[base : base + GROUP, :] = left
        inverse[base : base + GROUP, :] = right
        if base + GROUP < LEAF:
            both = jnp.concatenate([left, right], axis=1)
            high = both.astype(jnp.bfloat16).astype(jnp.float32)
            low = both - high
            keep = lanes >= base + GROUP
            lh, ll = [jnp.where(keep, v[:, :LEAF], 0.0) for v in (high, low)]
            update = lax.dot_general(
                jnp.concatenate([lh, ll, lh], axis=0), jnp.concatenate([high, high, low], axis=0),
                (((0,), (0,)), ((), ())), preferred_element_type=jnp.float32)
            aug[base + GROUP :, :] = aug[base + GROUP :, :] - update[base + GROUP :, :]


def remote(src, dst, send, recv, row, col):
    return pltpu.make_async_remote_copy(
        src_ref=src, dst_ref=dst, send_sem=send, recv_sem=recv,
        device_id=(row, col), device_id_type=MESH)


class Place:
    def __init__(self, n_rows, n_cols):
        self.n_rows, self.n_cols = n_rows, n_cols
        self.n_pos = n_rows // 2
        self.r = lax.axis_index("rows")
        self.c = lax.axis_index("cols")
        self.q = lax.div(self.r, 2)
        self.p = lax.rem(self.r, 2)
        self.partner = self.r + 1 - 2 * self.p
        self.far = lax.rem(self.c + 2, 4)
        self.near = self.c + 1 - 2 * lax.rem(self.c, 2)
        self.leads = self.q == 0
        self.follows = self.q >= 1
        self.passes = self.q + 1 < self.n_pos

    def barrier(self):
        sem = pltpu.get_barrier_semaphore()

        def greet(row, col):
            pl.semaphore_signal(sem, inc=1, device_id=(row, col), device_id_type=MESH)

        for i in range(1, self.n_cols):
            greet(self.r, lax.rem(self.c + i, self.n_cols))
        greet(self.partner, self.c)

        @pl.when(self.leads)
        def _():
            for s in range(1, self.n_pos):
                greet(self.r + 2 * s, self.c)
            pl.semaphore_wait(sem, self.n_cols + self.n_pos - 1)

        @pl.when(self.follows)
        def _():
            greet(self.p, self.c)

            @pl.when(self.q >= 2)
            def _():
                greet(self.r - 2, self.c)

            @pl.when(self.passes)
            def _():
                greet(self.r + 2, self.c)

            extra = (self.q >= 2).astype(jnp.int32) + self.passes.astype(jnp.int32)
            pl.semaphore_wait(sem, self.n_cols + 1 + extra)


class Blocks:
    def __init__(self, at, lower, pieces, sems):
        self.at, self.lower, self.pieces = at, lower, pieces
        self.row_send, self.row_recv, self.near_send, self.near_recv = sems

    def of(self, k):
        return [i for i, piece in enumerate(self.pieces) if piece[3] == k]

    def half(self, piece, owner):
        _, lo, size, k = self.pieces[piece]
        start = pl.multiple_of(lo + owner * (size // 2), 8)
        return self.lower.at[k, pl.ds(start, size // 2), :]

    def place(self, piece):
        return self.half(piece, lax.rem(self.at.c, 2))

    def to_row(self, piece, row):
        spot = self.place(piece)
        return remote(spot, spot, self.row_send.at[piece], self.row_recv.at[piece], row, self.at.c)

    def to_near(self, piece):
        spot = self.place(piece)
        return remote(spot, spot, self.near_send.at[piece], self.near_recv.at[piece], self.at.r, self.at.near)

    def near_in(self, piece):
        spot = self.half(piece, 1 - lax.rem(self.at.c, 2))
        return remote(spot, spot, self.near_send.at[piece], self.near_recv.at[piece], self.at.r, self.at.near)


class Raw(Blocks):
    def send(self, k):
        for piece in self.of(k):

            @pl.when(self.at.r == self.pieces[piece][0])
            def _():
                self.to_row(piece, self.at.partner).start()

    def come(self, piece):
        @pl.when(self.at.p != self.pieces[piece][0])
        def _():
            self.to_row(piece, self.at.partner).wait_recv()
            self.to_near(piece).start()

    def done(self, piece):
        @pl.when(self.at.p != self.pieces[piece][0])
        def _():
            self.near_in(piece).wait_recv()
            self.to_near(piece).wait_send()

        @pl.when(self.at.p == self.pieces[piece][0])
        def _():
            self.to_row(piece, self.at.partner).wait_send()


class Solved(Blocks):
    def __init__(self, at, lower, pieces, sems, straight=None):
        super().__init__(at, lower, pieces, sems)
        self.straight = straight

    def is_last(self, piece):
        return self.straight is not None and piece + 1 == len(self.pieces)

    def sends(self, piece):
        if not self.is_last(piece):
            return [self.to_row(piece, self.at.r + 2)]
        spot = self.place(piece)
        return [
            remote(spot, spot, self.straight.at[s - 1], self.row_recv.at[piece], self.at.r + 2 * s, self.at.c)
            for s in reversed(range(1, self.at.n_pos))
        ]

    def send(self, piece):
        for copy in self.sends(piece):
            copy.start()

    def sent(self, piece):
        for copy in self.sends(piece):
            copy.wait_send()

    def take(self, piece):
        self.to_row(piece, self.at.r + 2).wait_recv()
        if not self.is_last(piece):

            @pl.when(self.at.passes)
            def _():
                self.to_row(piece, self.at.r + 2).start()

        self.to_near(piece).start()

    def taken(self, piece):
        self.near_in(piece).wait_recv()

    def finish(self):
        for piece in range(len(self.pieces)):
            self.to_near(piece).wait_send()
            if not self.is_last(piece):

                @pl.when(self.at.passes)
                def _():
                    self.to_row(piece, self.at.r + 2).wait_send()


class Rows:
    def __init__(self, at, panel, own, target, gathered, staged, sems):
        self.at, self.panel, self.own, self.target = at, panel, own, target
        self.gathered, self.staged = gathered, staged
        (self.dn_send, self.dn_recv, self.up_send, self.up_recv, self.x_send, self.x_recv,
         self.t_send, self.t_recv, self.l_send, self.l_recv) = sems
        self.width = panel.shape[0]
        self.share = self.width // at.n_cols
        self.chunk = self.share // CHUNKS

    def part(self, ref, m, owner=None):
        owner = self.at.c if owner is None else owner
        start = pl.multiple_of(owner * self.share + m * self.chunk, 8)
        return ref.at[pl.ds(start, self.chunk), :]

    def chain(self, kind, s, m):
        at = self.at
        if kind == "dn":
            origin, dest, send, recv = at.r + 2 * (s - 1), at.r - 2, self.dn_send, self.dn_recv
        else:
            origin, dest, send, recv = at.r - 2 * (s - 1), at.r + 2, self.up_send, self.up_recv
        spot = self.gathered[m].at[origin]
        src = self.part(self.panel, m) if s == 1 else spot
        return remote(src, spot, send.at[s - 1, m], recv.at[s - 1, m], dest, at.c)

    def awaited(self, kind, s, m):
        at = self.at
        recv, send = (self.dn_recv, self.dn_send) if kind == "dn" else (self.up_recv, self.up_send)
        spot = self.gathered[m].at[at.r + 2 * s if kind == "dn" else at.r - 2 * s]
        return remote(spot, spot, send.at[s - 1, m], recv.at[s - 1, m], at.r, at.c)

    def across(self, origin, m, own):
        at = self.at
        spot = self.gathered[m].at[2 * origin + at.p]
        src = self.part(self.panel, m) if own else spot
        return remote(src, spot, self.x_send.at[origin, m], self.x_recv.at[origin, m], at.partner, at.c)

    def crossed(self, origin, m):
        at = self.at
        spot = self.gathered[m].at[2 * origin + 1 - at.p]
        return remote(spot, spot, self.x_send.at[origin, m], self.x_recv.at[origin, m], at.r, at.c)

    def open(self):
        at = self.at
        for m in range(CHUNKS):

            @pl.when(at.q >= 2)
            def _():
                self.chain("dn", 1, m).start()

            @pl.when(at.passes)
            def _():
                self.chain("up", 1, m).start()

            self.across(at.q, m, True).start()

    def keep_own(self):
        for m in range(CHUNKS):
            start = pl.multiple_of(self.at.c * self.share + m * self.chunk, 8)
            self.gathered[m][self.at.r] = self.own[pl.ds(start, self.chunk), :]

    def relay(self, s, m):
        at = self.at

        @pl.when(at.q + s < at.n_pos)
        def _():
            self.awaited("dn", s, m).wait_recv()
            self.across(at.q + s, m, False).start()

            @pl.when(at.q >= 2)
            def _():
                self.chain("dn", s + 1, m).start()

        @pl.when(at.q - s >= 1)
        def _():
            self.awaited("up", s, m).wait_recv()
            self.across(at.q - s, m, False).start()

            @pl.when(at.passes)
            def _():
                self.chain("up", s + 1, m).start()

    def select(self, m, rows, live):
        at = self.at
        for origin in range(1, at.n_pos):
            self.crossed(origin, m).wait_recv()
        start = pl.multiple_of(at.c * self.share + m * self.chunk, 8)
        for t in range(at.n_cols):
            value = self.gathered[m][rows[t]] * live[rows[t]].astype(jnp.float32)
            self.staged[m][t] = value

            @pl.when(at.c == t)
            def _():
                self.target[pl.ds(start, self.chunk), :] = value

    def deal(self, t, m):
        at = self.at
        return remote(self.staged[m].at[t], self.part(self.target, m), self.t_send.at[t, m],
                      self.t_recv.at[at.c, m], at.r, t)

    def deal_all(self, m):
        for t in range(self.at.n_cols):

            @pl.when(self.at.c != t)
            def _():
                self.deal(t, m).start()

    def to_leader(self, owner, m):
        at = self.at
        start = pl.multiple_of(owner * self.share + m * self.chunk, 8)
        rows = pl.ds(start, self.chunk)
        src = self.target.at[rows, pl.ds(pl.multiple_of(at.p * self.width, LEAF), self.width)]
        return remote(src, self.target.at[rows, pl.ds(0, self.width)], self.l_send.at[owner, m],
                      self.l_recv.at[owner, m], at.p, at.c)

    def dealt(self, m):
        at = self.at
        for i in range(1, at.n_cols):
            src = lax.rem(at.c + i, at.n_cols)
            spot = self.part(self.target, m, src)
            remote(spot, spot, self.t_send.at[src, m], self.t_recv.at[src, m], at.r, src).wait_recv()

        @pl.when(at.q == 1)
        def _():
            for owner in range(at.n_cols):
                self.to_leader(owner, m).start()

    def arrived(self):
        for m in range(CHUNKS):
            for owner in range(self.at.n_cols):
                self.to_leader(owner, m).wait_recv()

    def finish(self):
        at = self.at
        for m in range(CHUNKS):
            for t in range(at.n_cols):

                @pl.when(at.c != t)
                def _():
                    self.deal(t, m).wait_send()

                @pl.when(at.q == 1)
                def _():
                    self.to_leader(t, m).wait_send()

            for s in range(1, at.n_pos - 1):

                @pl.when((at.q >= 2) & (at.q + s - 1 < at.n_pos))
                def _():
                    self.chain("dn", s, m).wait_send()

                @pl.when(at.passes & (at.q - s + 1 >= 1))
                def _():
                    self.chain("up", s, m).wait_send()

            for origin in range(1, at.n_pos):
                self.across(origin, m, False).wait_send()


def lead(at, raw, solved, inverted, lower, split, inverses, aug, upper):
    total = lower.shape[1]
    n_leaf = total // LEAF
    rows = lax.broadcasted_iota(jnp.int32, (LEAF, LEAF), 0)
    lanes = lax.broadcasted_iota(jnp.int32, (LEAF, LEAF), 1)

    for b in range(1, n_leaf):
        lower[b, : b * LEAF, :] = jnp.zeros((b * LEAF, LEAF), jnp.float32)
    first = raw.of(0)
    raw.come(first[0])
    raw.done(first[0])

    def step(k, carry):
        here = pl.ds(pl.multiple_of(k * LEAF, LEAF), LEAF)
        block = lower[k, here, :]
        aug[:, :LEAF] = jnp.where(rows >= lanes, block, block.T)
        aug[:, LEAF:] = jnp.where(rows == lanes, 1.0, 0.0)
        factor_leaf(aug, upper, inverses.at[k])
        lower[k, here, :] = upper[...].T
        for b in range(n_leaf):

            @pl.when(k == b)
            def _():
                inverted.send(b)
                if b == 0:
                    for piece in first[1:] + raw.of(1) + raw.of(2):
                        raw.come(piece)
                    for piece in first[1:] + raw.of(1):
                        raw.done(piece)
                else:
                    if b + 2 < n_leaf:
                        for piece in raw.of(b + 2):
                            raw.come(piece)
                    if b + 1 < n_leaf:
                        for piece in raw.of(b + 1):
                            raw.done(piece)
                lo, hi = b * LEAF, (b + 1) * LEAF
                if hi < total:
                    column = times_trans(lower[b, hi:, :], inverses[b])
                    lower[b, hi:, :] = column
                    split.put(slice(hi, total), slice(lo, hi), column)
                    nxt = hi + LEAF
                    lower[b + 1, hi:, :] = lower[b + 1, hi:, :] - product(
                        split.get(slice(hi, total), slice(0, hi)), split.get(slice(hi, nxt), slice(0, hi)))
                    solved.send(b)

        return carry

    lax.fori_loop(0, n_leaf, step, 0)


def window_kernel(n_rows, n_cols, rows_in, live_in, panel, window, factor, other, updated,
                  window_rows, row_live, own, lower, target, inverses, aug, upper,
                  low_high, low_low, x_high, x_low, j_high, j_low, *rest):
    gathered, staged = rest[:CHUNKS], rest[CHUNKS : 2 * CHUNKS]
    own_sem, window_sem, rows_sem, live_sem, block_sem = rest[2 * CHUNKS : 2 * CHUNKS + 5]
    sems = rest[2 * CHUNKS + 5 :]
    at = Place(n_rows, n_cols)
    width = panel.shape[0]
    total = lower.shape[1]
    n_leaf = total // LEAF
    per = width // LEAF
    raw_pieces = [(0, 0, LEAF, 0), (0, LEAF, width - LEAF, 0)] + [
        (which, which * width + max(0, k - which * per) * LEAF, width - max(0, k - which * per) * LEAF, k)
        for k in range(n_leaf) for which in range(2) if k < (which + 1) * per and (k, which) != (0, 0)
    ]
    low_pieces = [(0, (k + 1) * LEAF, total - (k + 1) * LEAF, k) for k in range(n_leaf - 1)]
    raw = Raw(at, lower, raw_pieces, sems[1:5])
    solved = Solved(at, lower, low_pieces, sems[5:9])
    inv_pieces = [(0, 0, LEAF, k) for k in range(n_leaf)]
    inverted = Solved(at, inverses, inv_pieces, sems[9:13], sems[0])
    low_split, x_split = Split(low_high, low_low), Split(x_high, x_low)
    net = Rows(at, panel, own, target, gathered, staged, sems[13:])
    fetches = [
        pltpu.make_async_copy(window, updated, window_sem),
        pltpu.make_async_copy(rows_in, window_rows, rows_sem),
        pltpu.make_async_copy(live_in, row_live, live_sem),
    ]
    keep = pltpu.make_async_copy(panel, own, own_sem)

    def block_fetch(k):
        return pltpu.make_async_copy(
            panel.at[:, pl.ds(k * LEAF, LEAF)],
            lower.at[k, pl.ds(pl.multiple_of(at.p * width, LEAF), width), :], block_sem.at[k])

    @pl.when(at.leads)
    def _():
        for k in range(n_leaf):

            @pl.when(k < (at.p + 1) * per)
            def _():
                block_fetch(k).start()

    @pl.when(at.follows)
    def _():
        keep.start()

    for fetch in fetches:
        fetch.start()
    at.barrier()

    @pl.when(at.follows)
    def _():
        net.open()
        keep.wait()

    @pl.when(at.leads)
    def _():
        for k in range(n_leaf):

            @pl.when(k < (at.p + 1) * per)
            def _():
                block_fetch(k).wait()
                raw.send(k)

    for fetch in fetches:
        fetch.wait()
    live = row_live[at.r].astype(jnp.float32)

    @pl.when(at.leads)
    def _():
        lead(at, raw, solved, inverted, lower, low_split, inverses, aug, upper)
        for k in range(n_leaf):
            factor[:, k * LEAF : (k + 1) * LEAF] = lower[k, pl.ds(pl.multiple_of(at.p * width, width), width), :]
        for b in range(n_leaf):
            inverted.sent(b)
        for b in range(n_leaf - 1):
            solved.sent(b)
        net.arrived()
        updated[...] = updated[...] - target[:, :width].T

    @pl.when(at.follows)
    def _():
        net.keep_own()

        full = slice(0, width)
        j_split = Split(j_high, j_low)

        def span(b, count=1):
            return slice(b * LEAF, (b + count) * LEAF)

        def store(dst, split, b, value):
            dst[:, span(b)] = value
            split.put(full, span(b), value)

        for b in range(n_leaf):
            if b == 0:
                for s in range(1, at.n_pos - 2):
                    for m in range(CHUNKS):
                        net.relay(s, m)
            if b in (2, 3):
                for m in ((0, 1), (2, 3))[b - 2]:
                    net.relay(at.n_pos - 2, m)
            if 3 <= b < 3 + CHUNKS:
                net.select(b - 3, window_rows, row_live)
            if b:
                solved.take(b - 1)
            if 3 <= b < 3 + CHUNKS:
                net.deal_all(b - 3)
            if 5 <= b < 5 + CHUNKS:
                net.dealt(b - 5)
            now = own[:, span(b)] * live
            if b:
                solved.taken(b - 1)
                low_split.put(slice(b * LEAF, total), span(b - 1), lower[b - 1, b * LEAF :, :])
                now = now - product(x_split.get(full, span(0, b)), low_split.get(span(b), span(0, b)))
            if b == n_leaf - 1:
                factor[:, span(b)] = now
                net.dealt(CHUNKS - 1)
                for k in range(0, n_leaf, 2):
                    left, right = target[:, span(k)], target[:, span(k + 1)]
                    if k:
                        both = product(j_split.get(full, span(0, k)), low_split.get(span(k, 2), span(0, k)))
                        left, right = left - both[:, :LEAF], right - both[:, LEAF:]
                    store(other, j_split, k, times_trans(left, inverses[k]))
                    right = right - product(j_split.get(full, span(k)), low_split.get(span(k + 1), span(k)))
                    if k + 1 < b:
                        store(other, j_split, k + 1, times_trans(right, inverses[k + 1]))
                    else:
                        other[:, span(b)] = right
                updated[...] = updated[...] - product(x_split.get(full, span(0, b)), j_split.get(full, span(0, b)))
                now = factor[:, span(b)]
            inverted.take(b)
            inverted.taken(b)
            now = times_trans(now, inverses[b])
            if b == n_leaf - 1:
                factor[:, span(b)] = now
                other[:, span(b)] = times_trans(other[:, span(b)], inverses[b])
            else:
                store(factor, x_split, b, now)
        solved.finish()
        inverted.finish()
        net.finish()


def factor_window(window_rows, row_live, panel, window, n_rows, n_cols):
    if n_cols != 4 or n_rows < 6 or n_rows % 2:
        raise ValueError("unsupported mesh")
    width, total = panel.shape
    n_leaf = total // LEAF
    n_raw = n_leaf + width // LEAF + 1
    n_low = n_leaf - 1
    n_pos = n_rows // 2
    chunk = width // n_cols // CHUNKS
    dma = pltpu.SemaphoreType.DMA
    tall = jax.ShapeDtypeStruct(panel.shape, jnp.float32)
    return pl.pallas_call(
        functools.partial(window_kernel, n_rows, n_cols),
        out_shape=(tall, tall, jax.ShapeDtypeStruct(window.shape, jnp.float32)),
        in_specs=[pl.BlockSpec(memory_space=pltpu.HBM)] * 4,
        out_specs=(pl.BlockSpec(memory_space=pltpu.VMEM),) * 3,
        scratch_shapes=[
            pltpu.SMEM(window_rows.shape, jnp.int32),
            pltpu.SMEM(row_live.shape, jnp.int32),
            pltpu.VMEM(panel.shape, jnp.float32),
            pltpu.VMEM((n_leaf, total, LEAF), jnp.float32),
            pltpu.VMEM(panel.shape, jnp.float32),
            pltpu.VMEM((n_leaf, LEAF, LEAF), jnp.float32),
            pltpu.VMEM((LEAF, 2 * LEAF), jnp.float32),
            pltpu.VMEM((LEAF, LEAF), jnp.float32),
            pltpu.VMEM((total, total), jnp.bfloat16),
            pltpu.VMEM((total, total), jnp.bfloat16),
            pltpu.VMEM(panel.shape, jnp.bfloat16),
            pltpu.VMEM(panel.shape, jnp.bfloat16),
            pltpu.VMEM(panel.shape, jnp.bfloat16),
            pltpu.VMEM(panel.shape, jnp.bfloat16),
        ] + [pltpu.VMEM((n_rows, chunk, total), jnp.float32)] * CHUNKS
        + [pltpu.VMEM((n_cols, chunk, total), jnp.float32)] * CHUNKS
        + [
            dma(()), dma(()), dma(()), dma(()), dma((n_leaf,)),
            dma((n_pos - 1,)),
            dma((n_raw,)), dma((n_raw,)), dma((n_raw,)), dma((n_raw,)),
            dma((n_low,)), dma((n_low,)), dma((n_low,)), dma((n_low,)),
            dma((n_leaf,)), dma((n_leaf,)), dma((n_leaf,)), dma((n_leaf,)),
            dma((n_pos, CHUNKS)), dma((n_pos, CHUNKS)), dma((n_pos, CHUNKS)), dma((n_pos, CHUNKS)),
            dma((n_pos, CHUNKS)), dma((n_pos, CHUNKS)),
            dma((n_cols, CHUNKS)), dma((n_cols, CHUNKS)), dma((n_cols, CHUNKS)), dma((n_cols, CHUNKS)),
        ],
        compiler_params=pltpu.CompilerParams(
            collective_id=0, has_side_effects=True, vmem_limit_bytes=(29 << 20) + n_rows * n_cols * CHUNKS * chunk * total),
        cost_estimate=pl.CostEstimate(flops=10**10, bytes_accessed=10**7, transcendentals=0),
        name="factor_window",
    )(*[pltpu.with_memory_space_constraint(x, pltpu.HBM) for x in (window_rows, row_live, panel, window)])


def update_kernel(factor, other, partial, factor_out, updated, sem):
    store = pltpu.make_async_copy(factor, factor_out, sem)
    store.start()
    r = lax.axis_index("rows")
    lo = factor.shape[1] - LEAF

    @pl.when(r < P_SIZE)
    def _():
        updated[...] = partial[...]

    @pl.when(r >= P_SIZE)
    def _():
        updated[...] = partial[...] - times_trans(factor[:, lo:], other[:, lo:])

    store.wait()


def update_window(factor, other, partial):
    return pl.pallas_call(
        update_kernel,
        out_shape=(jax.ShapeDtypeStruct(factor.shape, jnp.float32),
                   jax.ShapeDtypeStruct(partial.shape, jnp.float32)),
        in_specs=[pl.BlockSpec(memory_space=pltpu.VMEM)] * 3,
        out_specs=(pl.BlockSpec(memory_space=pltpu.HBM), pl.BlockSpec(memory_space=pltpu.VMEM)),
        scratch_shapes=[pltpu.SemaphoreType.DMA(())],
        compiler_params=pltpu.CompilerParams(vmem_limit_bytes=24 << 20),
        cost_estimate=pl.CostEstimate(flops=10**9, bytes_accessed=10**7, transcendentals=0),
        name="update_window",
    )(factor, other, partial)


def shards(n_rows, n_cols, panel, window_block, row_live, window_rows):
    factor, other, partial = factor_window(window_rows, row_live, panel, window_block, n_rows, n_cols)
    return update_window(factor, other, partial)


def solution(mesh):
    in_specs = (P("rows", None), P("rows", "cols"), P(), P())
    out_specs = (P("rows", None), P("rows", "cols"))
    body = functools.partial(shards, mesh.shape["rows"], mesh.shape["cols"])
    return jax.shard_map(body, mesh=mesh, in_specs=in_specs, out_specs=out_specs, check_vma=False)
```

```python
import functools

import jax
import jax.numpy as jnp
from jax import lax
from jax.experimental import pallas as pl
from jax.experimental.pallas import tpu as pltpu
from jax.sharding import PartitionSpec as P

P_SIZE = 2
CONTRACT = (((1,), (1,)), ((), ()))
LEAF = 128
GROUP = 16
CHUNKS = 8
EARLY = 5
INV_STRAIGHT = 2
LOW_STRAIGHT = 1
LATE = {1: (0, 1), 2: (2, 3, 4), 3: (5, 6, 7)}
SELECT = {2: (0, 1), 3: (2, 3), 4: (4, 5), 5: (6, 7)}
DEALT = {4: (0, 1), 5: (2, 3), 6: (4, 5), 7: (6, 7)}
MESH = pl.DeviceIdType.MESH


def halves(value):
    high = value.astype(jnp.bfloat16)
    return high, (value - high.astype(jnp.float32)).astype(jnp.bfloat16)


def product(left, right):
    (lh, ll), (rh, rl) = left, right

    def dot(a, b):
        return lax.dot_general(a, b, CONTRACT, preferred_element_type=jnp.float32)

    return dot(lh, rh) + (dot(lh, rl) + dot(ll, rh))


def times_trans(left, right):
    return product(halves(left), halves(right))


class Split:
    def __init__(self, high, low):
        self.high, self.low = high, low

    def put(self, rows, cols, value):
        self.high[rows, cols], self.low[rows, cols] = halves(value)

    def get(self, rows, cols):
        return self.high[rows, cols], self.low[rows, cols]


def spread_row(value, k):
    return jnp.broadcast_to(value[k : k + 1, :], value.shape)


def factor_leaf(aug, upper, inverse):
    half = GROUP // 2
    subs = lax.broadcasted_iota(jnp.int32, (half, LEAF), 0)
    row_of = lax.broadcasted_iota(jnp.int32, (GROUP, LEAF), 1) - lax.broadcasted_iota(jnp.int32, (GROUP, LEAF), 0)
    lanes = lax.broadcasted_iota(jnp.int32, (GROUP, LEAF), 1)
    for g in range(LEAF // GROUP):
        base = g * GROUP
        parts = [[aug[base + h * half : base + (h + 1) * half, s * LEAF : (s + 1) * LEAF] for s in range(2)]
                 for h in range(2)]
        cols = [[jnp.broadcast_to(parts[h][0][:, base + j : base + j + 1], (half, LEAF)) for j in range(GROUP)]
                for h in range(2)]
        scales = [jnp.zeros((half, LEAF), jnp.float32)] * 2
        for k in range(GROUP):
            h, kk = k // half, k % half
            root = lax.rsqrt(spread_row(cols[h][k], kk))
            scales[h] = jnp.where(subs == kk, root, scales[h])
            if k + 1 == GROUP:
                break
            inv = root * root
            mults = {i: cols[i][k] * inv for i in range(h, 2)}
            for j in range(k + 1, GROUP):
                row = spread_row(cols[h][j], kk)
                for i in range(h, 2):
                    cols[i][j] = cols[i][j] - mults[i] * row
            mults[h] = jnp.where(subs > kk, mults[h], 0.0)
            for s in range(2):
                row = spread_row(parts[h][s], kk)
                for i in range(h, 2):
                    parts[i][s] = parts[i][s] - mults[i] * row
        left = jnp.concatenate([parts[h][0] * scales[h] for h in range(2)], axis=0)
        right = jnp.concatenate([parts[h][1] * scales[h] for h in range(2)], axis=0)
        left = jnp.where(row_of >= base, left, 0.0)
        upper[base : base + GROUP, :] = left
        inverse[base : base + GROUP, :] = right
        if base + GROUP < LEAF:
            both = jnp.concatenate([left, right], axis=1)
            high = both.astype(jnp.bfloat16).astype(jnp.float32)
            low = both - high
            keep = lanes >= base + GROUP
            lh, ll = [jnp.where(keep, v[:, :LEAF], 0.0) for v in (high, low)]
            update = lax.dot_general(
                jnp.concatenate([lh, ll, lh], axis=0), jnp.concatenate([high, high, low], axis=0),
                (((0,), (0,)), ((), ())), preferred_element_type=jnp.float32)
            aug[base + GROUP :, :] = aug[base + GROUP :, :] - update[base + GROUP :, :]


def remote(src, dst, send, recv, row, col):
    return pltpu.make_async_remote_copy(
        src_ref=src, dst_ref=dst, send_sem=send, recv_sem=recv,
        device_id=(row, col), device_id_type=MESH)


class Place:
    def __init__(self, n_rows, n_cols):
        self.n_rows, self.n_cols = n_rows, n_cols
        self.n_pos = n_rows // 2
        self.r = lax.axis_index("rows")
        self.c = lax.axis_index("cols")
        self.q = lax.div(self.r, 2)
        self.p = lax.rem(self.r, 2)
        self.partner = self.r + 1 - 2 * self.p
        self.far = lax.rem(self.c + 2, 4)
        self.near = self.c + 1 - 2 * lax.rem(self.c, 2)
        self.leads = self.q == 0
        self.follows = self.q >= 1
        self.passes = self.q + 1 < self.n_pos

    def barrier(self):
        sem = pltpu.get_barrier_semaphore()

        def greet(row, col):
            pl.semaphore_signal(sem, inc=1, device_id=(row, col), device_id_type=MESH)

        for i in range(1, self.n_cols):
            greet(self.r, lax.rem(self.c + i, self.n_cols))
        greet(self.partner, self.c)

        @pl.when(self.leads)
        def _():
            for s in range(1, self.n_pos):
                greet(self.r + 2 * s, self.c)
            for i in range(1, self.n_cols):
                greet(self.r + 2, lax.rem(self.c + i, self.n_cols))
            pl.semaphore_wait(sem, 2 * self.n_cols + self.n_pos - 2)

        @pl.when(self.follows)
        def _():
            greet(self.p, self.c)

            @pl.when(self.q == 1)
            def _():
                for i in range(1, self.n_cols):
                    greet(self.p, lax.rem(self.c + i, self.n_cols))

            @pl.when(self.q >= 2)
            def _():
                greet(self.r - 2, self.c)

            @pl.when(self.passes)
            def _():
                greet(self.r + 2, self.c)

            first = (self.q == 1).astype(jnp.int32)
            extra = first * (self.n_cols - 1) + (1 - first) + self.passes.astype(jnp.int32)
            pl.semaphore_wait(sem, self.n_cols + 1 + extra)


class Blocks:
    def __init__(self, at, lower, pieces, sems):
        self.at, self.lower, self.pieces = at, lower, pieces
        self.row_send, self.row_recv, self.near_send, self.near_recv = sems

    def of(self, k):
        return [i for i, piece in enumerate(self.pieces) if piece[3] == k]

    def half(self, piece, owner):
        _, lo, size, k = self.pieces[piece]
        start = pl.multiple_of(lo + owner * (size // 2), 8)
        return self.lower.at[k, pl.ds(start, size // 2), :]

    def place(self, piece):
        return self.half(piece, lax.rem(self.at.c, 2))

    def to_row(self, piece, row):
        spot = self.place(piece)
        return remote(spot, spot, self.row_send.at[piece], self.row_recv.at[piece], row, self.at.c)

    def to_near(self, piece):
        spot = self.place(piece)
        return remote(spot, spot, self.near_send.at[piece], self.near_recv.at[piece], self.at.r, self.at.near)

    def near_in(self, piece):
        spot = self.half(piece, 1 - lax.rem(self.at.c, 2))
        return remote(spot, spot, self.near_send.at[piece], self.near_recv.at[piece], self.at.r, self.at.near)


class Raw(Blocks):
    def send(self, k):
        for piece in self.of(k):

            @pl.when(self.at.r == self.pieces[piece][0])
            def _():
                self.to_row(piece, self.at.partner).start()

    def come(self, piece):
        @pl.when(self.at.p != self.pieces[piece][0])
        def _():
            self.to_row(piece, self.at.partner).wait_recv()
            self.to_near(piece).start()

    def done(self, piece):
        @pl.when(self.at.p != self.pieces[piece][0])
        def _():
            self.near_in(piece).wait_recv()
            self.to_near(piece).wait_send()

        @pl.when(self.at.p == self.pieces[piece][0])
        def _():
            self.to_row(piece, self.at.partner).wait_send()


class Solved(Blocks):
    def __init__(self, at, lower, pieces, sems, straight, n_straight):
        super().__init__(at, lower, pieces, sems)
        self.straight = straight
        self.first_straight = len(pieces) - n_straight

    def is_last(self, piece):
        return piece >= self.first_straight

    def sends(self, piece):
        if not self.is_last(piece):
            return [self.to_row(piece, self.at.r + 2)]
        spot = self.place(piece)
        return [
            remote(spot, spot, self.straight.at[piece - self.first_straight, s - 1], self.row_recv.at[piece], self.at.r + 2 * s, self.at.c)
            for s in reversed(range(1, self.at.n_pos))
        ]

    def send(self, piece):
        for copy in self.sends(piece):
            copy.start()

    def sent(self, piece):
        for copy in self.sends(piece):
            copy.wait_send()

    def take(self, piece):
        self.to_row(piece, self.at.r + 2).wait_recv()
        if not self.is_last(piece):

            @pl.when(self.at.passes)
            def _():
                self.to_row(piece, self.at.r + 2).start()

        self.to_near(piece).start()

    def taken(self, piece):
        self.near_in(piece).wait_recv()

    def finish(self):
        for piece in range(len(self.pieces)):
            self.to_near(piece).wait_send()
            if not self.is_last(piece):

                @pl.when(self.at.passes)
                def _():
                    self.to_row(piece, self.at.r + 2).wait_send()


class Rows:
    def __init__(self, at, panel, own, target, gathered, staged, sems):
        self.at, self.panel, self.own, self.target = at, panel, own, target
        self.gathered, self.staged = gathered, staged
        (self.dn_send, self.dn_recv, self.up_send, self.up_recv, self.x_send, self.x_recv,
         self.t_send, self.t_recv, self.l_send, self.l_recv) = sems
        self.width = panel.shape[0]
        self.share = self.width // at.n_cols
        self.chunk = self.share // CHUNKS

    def part(self, ref, m, owner=None):
        owner = self.at.c if owner is None else owner
        start = pl.multiple_of(owner * self.share + m * self.chunk, 8)
        return ref.at[pl.ds(start, self.chunk), :]

    def chain(self, kind, s, m):
        at = self.at
        if kind == "dn":
            origin, dest, send, recv = at.r + 2 * (s - 1), at.r - 2, self.dn_send, self.dn_recv
        else:
            origin, dest, send, recv = at.r - 2 * (s - 1), at.r + 2, self.up_send, self.up_recv
        spot = self.gathered[m].at[origin]
        src = self.part(self.panel, m) if s == 1 else spot
        return remote(src, spot, send.at[s - 1, m], recv.at[s - 1, m], dest, at.c)

    def awaited(self, kind, s, m):
        at = self.at
        recv, send = (self.dn_recv, self.dn_send) if kind == "dn" else (self.up_recv, self.up_send)
        spot = self.gathered[m].at[at.r + 2 * s if kind == "dn" else at.r - 2 * s]
        return remote(spot, spot, send.at[s - 1, m], recv.at[s - 1, m], at.r, at.c)

    def across(self, origin, m, own):
        at = self.at
        spot = self.gathered[m].at[2 * origin + at.p]
        src = self.part(self.panel, m) if own else spot
        return remote(src, spot, self.x_send.at[origin, m], self.x_recv.at[origin, m], at.partner, at.c)

    def crossed(self, origin, m):
        at = self.at
        spot = self.gathered[m].at[2 * origin + 1 - at.p]
        return remote(spot, spot, self.x_send.at[origin, m], self.x_recv.at[origin, m], at.r, at.c)

    def open(self):
        at = self.at
        for m in range(CHUNKS):

            @pl.when(at.q >= 2)
            def _():
                self.chain("dn", 1, m).start()

            @pl.when(at.passes)
            def _():
                self.chain("up", 1, m).start()

    def keep_own(self):
        for m in range(CHUNKS):
            start = pl.multiple_of(self.at.c * self.share + m * self.chunk, 8)
            self.gathered[m][self.at.r] = self.own[pl.ds(start, self.chunk), :]

    def relay(self, s, m):
        at = self.at

        @pl.when(at.q + s < at.n_pos)
        def _():
            self.awaited("dn", s, m).wait_recv()

            @pl.when(at.q >= 2)
            def _():
                self.chain("dn", s + 1, m).start()

        @pl.when(at.q - s >= 1)
        def _():
            self.awaited("up", s, m).wait_recv()

            @pl.when(at.passes)
            def _():
                self.chain("up", s + 1, m).start()

    def cross(self, s, m):
        at = self.at
        if s == 0:
            self.across(at.q, m, True).start()
            return

        @pl.when(at.q + s < at.n_pos)
        def _():
            self.across(at.q + s, m, False).start()

        @pl.when(at.q - s >= 1)
        def _():
            self.across(at.q - s, m, False).start()

    def select(self, m, rows, live):
        at = self.at
        for origin in range(1, at.n_pos):
            self.crossed(origin, m).wait_recv()
        start = pl.multiple_of(at.c * self.share + m * self.chunk, 8)
        for t in range(at.n_cols):
            value = self.gathered[m][rows[t]] * live[rows[t]].astype(jnp.float32)
            self.staged[m][t] = value

            @pl.when(at.c == t)
            def _():
                self.target[pl.ds(start, self.chunk), :] = value

    def deal(self, t, m):
        at = self.at
        return remote(self.staged[m].at[t], self.part(self.target, m), self.t_send.at[t, m],
                      self.t_recv.at[at.c, m], at.r, t)

    def deal_all(self, m):
        for t in range(self.at.n_cols):

            @pl.when(self.at.c != t)
            def _():
                self.deal(t, m).start()

            @pl.when(self.at.q == 1)
            def _():
                self.to_leader(t, m).start()

    def to_leader(self, t, m):
        at = self.at
        cols = pl.ds(pl.multiple_of(at.p * self.width, LEAF), self.width)
        return remote(self.staged[m].at[t, :, cols], self.left_part(m, at.c), self.l_send.at[t, m],
                      self.l_recv.at[at.c, m], at.p, t)

    def left_part(self, m, owner):
        start = pl.multiple_of(owner * self.share + m * self.chunk, 8)
        return self.target.at[pl.ds(start, self.chunk), pl.ds(0, self.width)]

    def dealt(self, m):
        at = self.at
        for i in range(1, at.n_cols):
            src = lax.rem(at.c + i, at.n_cols)
            spot = self.part(self.target, m, src)
            remote(spot, spot, self.t_send.at[src, m], self.t_recv.at[src, m], at.r, src).wait_recv()

    def arrived(self):
        for m in range(CHUNKS):
            for owner in range(self.at.n_cols):
                spot = self.left_part(m, owner)
                remote(spot, spot, self.l_send.at[owner, m], self.l_recv.at[owner, m],
                       self.at.r, self.at.c).wait_recv()

    def finish(self):
        at = self.at
        for m in range(CHUNKS):
            for t in range(at.n_cols):

                @pl.when(at.c != t)
                def _():
                    self.deal(t, m).wait_send()

                @pl.when(at.q == 1)
                def _():
                    self.to_leader(t, m).wait_send()

            for s in range(1, at.n_pos - 1):

                @pl.when((at.q >= 2) & (at.q + s - 1 < at.n_pos))
                def _():
                    self.chain("dn", s, m).wait_send()

                @pl.when(at.passes & (at.q - s + 1 >= 1))
                def _():
                    self.chain("up", s, m).wait_send()

            for origin in range(1, at.n_pos):
                self.across(origin, m, False).wait_send()


def lead(at, raw, solved, inverted, lower, split, inverses, aug, upper):
    total = lower.shape[1]
    n_leaf = total // LEAF
    rows = lax.broadcasted_iota(jnp.int32, (LEAF, LEAF), 0)
    lanes = lax.broadcasted_iota(jnp.int32, (LEAF, LEAF), 1)

    for b in range(1, n_leaf):
        lower[b, : b * LEAF, :] = jnp.zeros((b * LEAF, LEAF), jnp.float32)
    first = raw.of(0)
    raw.come(first[0])
    raw.done(first[0])

    def step(k, carry):
        here = pl.ds(pl.multiple_of(k * LEAF, LEAF), LEAF)
        block = lower[k, here, :]
        aug[:, :LEAF] = jnp.where(rows >= lanes, block, block.T)
        aug[:, LEAF:] = jnp.where(rows == lanes, 1.0, 0.0)
        factor_leaf(aug, upper, inverses.at[k])
        lower[k, here, :] = upper[...].T
        for b in range(n_leaf):

            @pl.when(k == b)
            def _():
                inverted.send(b)
                if b == 0:
                    for piece in first[1:] + raw.of(1) + raw.of(2):
                        raw.come(piece)
                    for piece in first[1:] + raw.of(1):
                        raw.done(piece)
                else:
                    if b + 2 < n_leaf:
                        for piece in raw.of(b + 2):
                            raw.come(piece)
                    if b + 1 < n_leaf:
                        for piece in raw.of(b + 1):
                            raw.done(piece)
                lo, hi = b * LEAF, (b + 1) * LEAF
                if hi < total:
                    column = times_trans(lower[b, hi:, :], inverses[b])
                    lower[b, hi:, :] = column
                    split.put(slice(hi, total), slice(lo, hi), column)
                    nxt = hi + LEAF
                    lower[b + 1, hi:, :] = lower[b + 1, hi:, :] - product(
                        split.get(slice(hi, total), slice(0, hi)), split.get(slice(hi, nxt), slice(0, hi)))
                    solved.send(b)

        return carry

    lax.fori_loop(0, n_leaf, step, 0)


def window_kernel(n_rows, n_cols, rows_in, live_in, panel, window, factor, other, updated,
                  window_rows, row_live, own, lower, target, inverses, aug, upper,
                  low_high, low_low, x_high, x_low, j_high, j_low, *rest):
    gathered, staged = rest[:CHUNKS], rest[CHUNKS : 2 * CHUNKS]
    own_sem, window_sem, rows_sem, live_sem, block_sem = rest[2 * CHUNKS : 2 * CHUNKS + 5]
    sems = rest[2 * CHUNKS + 5 :]
    at = Place(n_rows, n_cols)
    width = panel.shape[0]
    total = lower.shape[1]
    n_leaf = total // LEAF
    per = width // LEAF
    raw_pieces = [(0, 0, LEAF, 0), (0, LEAF, width - LEAF, 0)] + [
        (which, which * width + max(0, k - which * per) * LEAF, width - max(0, k - which * per) * LEAF, k)
        for k in range(n_leaf) for which in range(2) if k < (which + 1) * per and (k, which) != (0, 0)
    ]
    low_pieces = [(0, (k + 1) * LEAF, total - (k + 1) * LEAF, k) for k in range(n_leaf - 1)]
    raw = Raw(at, lower, raw_pieces, sems[2:6])
    solved = Solved(at, lower, low_pieces, sems[6:10], sems[1], LOW_STRAIGHT)
    inv_pieces = [(0, 0, LEAF, k) for k in range(n_leaf)]
    inverted = Solved(at, inverses, inv_pieces, sems[10:14], sems[0], INV_STRAIGHT)
    low_split, x_split = Split(low_high, low_low), Split(x_high, x_low)
    net = Rows(at, panel, own, target, gathered, staged, sems[14:])
    fetches = [
        pltpu.make_async_copy(window, updated, window_sem),
        pltpu.make_async_copy(rows_in, window_rows, rows_sem),
        pltpu.make_async_copy(live_in, row_live, live_sem),
    ]
    keep = pltpu.make_async_copy(panel, own, own_sem)

    def block_fetch(k):
        return pltpu.make_async_copy(
            panel.at[:, pl.ds(k * LEAF, LEAF)],
            lower.at[k, pl.ds(pl.multiple_of(at.p * width, LEAF), width), :], block_sem.at[k])

    @pl.when(at.leads)
    def _():
        for k in range(n_leaf):

            @pl.when(k < (at.p + 1) * per)
            def _():
                block_fetch(k).start()

    @pl.when(at.follows)
    def _():
        keep.start()

    for fetch in fetches:
        fetch.start()
    at.barrier()

    @pl.when(at.follows)
    def _():
        net.open()
        keep.wait()

    @pl.when(at.leads)
    def _():
        for k in range(n_leaf):

            @pl.when(k < (at.p + 1) * per)
            def _():
                block_fetch(k).wait()
                raw.send(k)

    for fetch in fetches:
        fetch.wait()
    live = row_live[at.r].astype(jnp.float32)

    @pl.when(at.leads)
    def _():
        lead(at, raw, solved, inverted, lower, low_split, inverses, aug, upper)
        for k in range(n_leaf):
            factor[:, k * LEAF : (k + 1) * LEAF] = lower[k, pl.ds(pl.multiple_of(at.p * width, width), width), :]
        for b in range(n_leaf):
            inverted.sent(b)
        for b in range(n_leaf - 1):
            solved.sent(b)
        net.arrived()
        updated[...] = updated[...] - target[:, :width].T

    @pl.when(at.follows)
    def _():
        net.keep_own()

        full = slice(0, width)
        j_split = Split(j_high, j_low)

        def span(b, count=1):
            return slice(b * LEAF, (b + count) * LEAF)

        def store(dst, split, b, value):
            dst[:, span(b)] = value
            split.put(full, span(b), value)

        share = width // n_cols
        halves_of = [[slice(c * share + h * share // 2, c * share + (h + 1) * share // 2) for c in range(n_cols)]
                     for h in range(2)]

        def gather(ref, h, cols):
            return jnp.concatenate([ref[rows, cols] for rows in halves_of[h]], axis=0)

        def scatter(ref, h, cols, value):
            size = share // 2
            for i, rows in enumerate(halves_of[h]):
                ref[rows, cols] = value[i * size : (i + 1) * size]

        def keep_j(h, b, value):
            scatter(other, h, span(b), value)
            for ref, part in zip((j_high, j_low), halves(value)):
                scatter(ref, h, span(b), part)

        def window_rows_step(h, k):
            def j_get(cols):
                return gather(j_high, h, cols), gather(j_low, h, cols)

            left, right = gather(target, h, span(k)), gather(target, h, span(k + 1))
            if k:
                both = product(j_get(span(0, k)), low_split.get(span(k, 2), span(0, k)))
                left, right = left - both[:, :LEAF], right - both[:, LEAF:]
            left = times_trans(left, inverses[k])
            keep_j(h, k, left)
            right = right - product(halves(left), low_split.get(span(k + 1), span(k)))
            if k + 2 < n_leaf:
                keep_j(h, k + 1, times_trans(right, inverses[k + 1]))
            else:
                scatter(other, h, span(k + 1), right)

        def cross(m):
            for s in range(at.n_pos - 2):
                net.cross(s, m)

        for b in range(n_leaf):
            if b == 0:
                for m in range(CHUNKS):
                    for s in range(1, at.n_pos - 2):
                        net.relay(s, m)
                    if m < EARLY:
                        cross(m)
            if b == n_leaf - 2:
                for k in range(0, n_leaf - 2, 2):
                    window_rows_step(0, k)
            for m in LATE.get(b, ()):
                net.relay(at.n_pos - 2, m)
                net.cross(at.n_pos - 2, m)
            if b and EARLY + b - 1 < CHUNKS:
                cross(EARLY + b - 1)
            for m in SELECT.get(b, ()):
                net.select(m, window_rows, row_live)
            if b + 1 < n_leaf:
                inverted.take(b)
            for m in SELECT.get(b, ()):
                net.deal_all(m)
            if b:
                solved.taken(b - 1)
                low_split.put(slice(b * LEAF, total), span(b - 1), lower[b - 1, b * LEAF :, :])
            if b % 2:
                now = factor[:, span(b)] - product(
                    x_split.get(full, span(b - 1)), low_split.get(span(b), span(b - 1)))
            else:
                pair = own[:, span(b, 2)] * live
                if b:
                    pair = pair - product(x_split.get(full, span(0, b)), low_split.get(span(b, 2), span(0, b)))
                now = pair[:, :LEAF]
                factor[:, span(b + 1)] = pair[:, LEAF:]
            for m in DEALT.get(b, ()):
                net.dealt(m)
            if b == n_leaf - 1:
                factor[:, span(b)] = now
                for k in range(0, n_leaf - 2, 2):
                    window_rows_step(1, k)
                window_rows_step(0, n_leaf - 2)
                window_rows_step(1, n_leaf - 2)
                updated[...] = updated[...] - product(x_split.get(full, span(0, b)), j_split.get(full, span(0, b)))
                now = factor[:, span(b)]
            if b + 1 == n_leaf:
                inverted.take(b)
            inverted.taken(b)
            now = times_trans(now, inverses[b])
            if b == n_leaf - 1:
                factor[:, span(b)] = now
                other[:, span(b)] = times_trans(other[:, span(b)], inverses[b])
            else:
                store(factor, x_split, b, now)
                solved.take(b)
        solved.finish()
        inverted.finish()
        net.finish()


def factor_window(window_rows, row_live, panel, window, n_rows, n_cols):
    if n_cols != 4 or n_rows < 6 or n_rows % 2:
        raise ValueError("unsupported mesh")
    width, total = panel.shape
    n_leaf = total // LEAF
    n_raw = n_leaf + width // LEAF + 1
    n_low = n_leaf - 1
    n_pos = n_rows // 2
    chunk = width // n_cols // CHUNKS
    dma = pltpu.SemaphoreType.DMA
    tall = jax.ShapeDtypeStruct(panel.shape, jnp.float32)
    return pl.pallas_call(
        functools.partial(window_kernel, n_rows, n_cols),
        out_shape=(tall, tall, jax.ShapeDtypeStruct(window.shape, jnp.float32)),
        in_specs=[pl.BlockSpec(memory_space=pltpu.HBM)] * 4,
        out_specs=(pl.BlockSpec(memory_space=pltpu.VMEM),) * 3,
        scratch_shapes=[
            pltpu.SMEM(window_rows.shape, jnp.int32),
            pltpu.SMEM(row_live.shape, jnp.int32),
            pltpu.VMEM(panel.shape, jnp.float32),
            pltpu.VMEM((n_leaf, total, LEAF), jnp.float32),
            pltpu.VMEM(panel.shape, jnp.float32),
            pltpu.VMEM((n_leaf, LEAF, LEAF), jnp.float32),
            pltpu.VMEM((LEAF, 2 * LEAF), jnp.float32),
            pltpu.VMEM((LEAF, LEAF), jnp.float32),
            pltpu.VMEM((total, total), jnp.bfloat16),
            pltpu.VMEM((total, total), jnp.bfloat16),
            pltpu.VMEM(panel.shape, jnp.bfloat16),
            pltpu.VMEM(panel.shape, jnp.bfloat16),
            pltpu.VMEM(panel.shape, jnp.bfloat16),
            pltpu.VMEM(panel.shape, jnp.bfloat16),
        ] + [pltpu.VMEM((n_rows, chunk, total), jnp.float32)] * CHUNKS
        + [pltpu.VMEM((n_cols, chunk, total), jnp.float32)] * CHUNKS
        + [
            dma(()), dma(()), dma(()), dma(()), dma((n_leaf,)),
            dma((INV_STRAIGHT, n_pos - 1)), dma((LOW_STRAIGHT, n_pos - 1)),
            dma((n_raw,)), dma((n_raw,)), dma((n_raw,)), dma((n_raw,)),
            dma((n_low,)), dma((n_low,)), dma((n_low,)), dma((n_low,)),
            dma((n_leaf,)), dma((n_leaf,)), dma((n_leaf,)), dma((n_leaf,)),
            dma((n_pos, CHUNKS)), dma((n_pos, CHUNKS)), dma((n_pos, CHUNKS)), dma((n_pos, CHUNKS)),
            dma((n_pos, CHUNKS)), dma((n_pos, CHUNKS)),
            dma((n_cols, CHUNKS)), dma((n_cols, CHUNKS)), dma((n_cols, CHUNKS)), dma((n_cols, CHUNKS)),
        ],
        compiler_params=pltpu.CompilerParams(
            collective_id=0, has_side_effects=True, vmem_limit_bytes=(29 << 20) + n_rows * n_cols * CHUNKS * chunk * total),
        cost_estimate=pl.CostEstimate(flops=10**10, bytes_accessed=10**7, transcendentals=0),
        name="factor_window",
    )(*[pltpu.with_memory_space_constraint(x, pltpu.HBM) for x in (window_rows, row_live, panel, window)])


def update_kernel(factor, other, partial, factor_out, updated, sem):
    store = pltpu.make_async_copy(factor, factor_out, sem)
    store.start()
    r = lax.axis_index("rows")
    lo = factor.shape[1] - LEAF

    @pl.when(r < P_SIZE)
    def _():
        updated[...] = partial[...]

    @pl.when(r >= P_SIZE)
    def _():
        updated[...] = partial[...] - times_trans(factor[:, lo:], other[:, lo:])

    store.wait()


def update_window(factor, other, partial):
    return pl.pallas_call(
        update_kernel,
        out_shape=(jax.ShapeDtypeStruct(factor.shape, jnp.float32),
                   jax.ShapeDtypeStruct(partial.shape, jnp.float32)),
        in_specs=[pl.BlockSpec(memory_space=pltpu.VMEM)] * 3,
        out_specs=(pl.BlockSpec(memory_space=pltpu.HBM), pl.BlockSpec(memory_space=pltpu.VMEM)),
        scratch_shapes=[pltpu.SemaphoreType.DMA(())],
        compiler_params=pltpu.CompilerParams(vmem_limit_bytes=24 << 20),
        cost_estimate=pl.CostEstimate(flops=10**9, bytes_accessed=10**7, transcendentals=0),
        name="update_window",
    )(factor, other, partial)


def shards(n_rows, n_cols, panel, window_block, row_live, window_rows):
    factor, other, partial = factor_window(window_rows, row_live, panel, window_block, n_rows, n_cols)
    return update_window(factor, other, partial)


def solution(mesh):
    in_specs = (P("rows", None), P("rows", "cols"), P(), P())
    out_specs = (P("rows", None), P("rows", "cols"))
    body = functools.partial(shards, mesh.shape["rows"], mesh.shape["cols"])
    return jax.shard_map(body, mesh=mesh, in_specs=in_specs, out_specs=out_specs, check_vma=False)
```

```python
import functools

import jax
import jax.numpy as jnp
from jax import lax
from jax.experimental import pallas as pl
from jax.experimental.pallas import tpu as pltpu
from jax.sharding import PartitionSpec as P

P_SIZE = 2
CONTRACT = (((1,), (1,)), ((), ()))
LEAF = 128
GROUP = 16
CHUNKS = 8
EARLY = 6
INV_STRAIGHT = 2
LOW_STRAIGHT = 1
LATE = {1: (0, 1, 2), 2: (3, 4, 5), 3: (6, 7)}
SELECT = {2: (0, 1), 3: (2, 3), 4: (4, 5), 5: (6, 7)}
DEALT = {4: (0, 1), 5: (2, 3), 6: (4, 5), 7: (6, 7)}
MESH = pl.DeviceIdType.MESH


def halves(value):
    high = value.astype(jnp.bfloat16)
    return high, (value - high.astype(jnp.float32)).astype(jnp.bfloat16)


def product(left, right):
    (lh, ll), (rh, rl) = left, right

    def dot(a, b):
        return lax.dot_general(a, b, CONTRACT, preferred_element_type=jnp.float32)

    return dot(lh, rh) + (dot(lh, rl) + dot(ll, rh))


def times_trans(left, right):
    return product(halves(left), halves(right))


class Split:
    def __init__(self, high, low):
        self.high, self.low = high, low

    def put(self, rows, cols, value):
        self.high[rows, cols], self.low[rows, cols] = halves(value)

    def get(self, rows, cols):
        return self.high[rows, cols], self.low[rows, cols]


def spread_row(value, k):
    return jnp.broadcast_to(value[k : k + 1, :], value.shape)


def factor_leaf(aug, upper, inverse):
    half = GROUP // 2
    subs = lax.broadcasted_iota(jnp.int32, (half, LEAF), 0)
    row_of = lax.broadcasted_iota(jnp.int32, (GROUP, LEAF), 1) - lax.broadcasted_iota(jnp.int32, (GROUP, LEAF), 0)
    lanes = lax.broadcasted_iota(jnp.int32, (GROUP, LEAF), 1)
    for g in range(LEAF // GROUP):
        base = g * GROUP
        parts = [[aug[base + h * half : base + (h + 1) * half, s * LEAF : (s + 1) * LEAF] for s in range(2)]
                 for h in range(2)]
        cols = [[jnp.broadcast_to(parts[h][0][:, base + j : base + j + 1], (half, LEAF)) for j in range(GROUP)]
                for h in range(2)]
        scales = [jnp.zeros((half, LEAF), jnp.float32)] * 2
        for k in range(GROUP):
            h, kk = k // half, k % half
            root = lax.rsqrt(spread_row(cols[h][k], kk))
            scales[h] = jnp.where(subs == kk, root, scales[h])
            if k + 1 == GROUP:
                break
            inv = root * root
            mults = {i: cols[i][k] * inv for i in range(h, 2)}
            for j in range(k + 1, GROUP):
                row = spread_row(cols[h][j], kk)
                for i in range(h, 2):
                    cols[i][j] = cols[i][j] - mults[i] * row
            mults[h] = jnp.where(subs > kk, mults[h], 0.0)
            for s in range(2):
                row = spread_row(parts[h][s], kk)
                for i in range(h, 2):
                    parts[i][s] = parts[i][s] - mults[i] * row
        left = jnp.concatenate([parts[h][0] * scales[h] for h in range(2)], axis=0)
        right = jnp.concatenate([parts[h][1] * scales[h] for h in range(2)], axis=0)
        left = jnp.where(row_of >= base, left, 0.0)
        upper[base : base + GROUP, :] = left
        inverse[base : base + GROUP, :] = right
        if base + GROUP < LEAF:
            both = jnp.concatenate([left, right], axis=1)
            high = both.astype(jnp.bfloat16).astype(jnp.float32)
            low = both - high
            keep = lanes >= base + GROUP
            lh, ll = [jnp.where(keep, v[:, :LEAF], 0.0) for v in (high, low)]
            update = lax.dot_general(
                jnp.concatenate([lh, ll, lh], axis=0), jnp.concatenate([high, high, low], axis=0),
                (((0,), (0,)), ((), ())), preferred_element_type=jnp.float32)
            aug[base + GROUP :, :] = aug[base + GROUP :, :] - update[base + GROUP :, :]


def remote(src, dst, send, recv, row, col):
    return pltpu.make_async_remote_copy(
        src_ref=src, dst_ref=dst, send_sem=send, recv_sem=recv,
        device_id=(row, col), device_id_type=MESH)


class Place:
    def __init__(self, n_rows, n_cols):
        self.n_rows, self.n_cols = n_rows, n_cols
        self.n_pos = n_rows // 2
        self.r = lax.axis_index("rows")
        self.c = lax.axis_index("cols")
        self.q = lax.div(self.r, 2)
        self.p = lax.rem(self.r, 2)
        self.partner = self.r + 1 - 2 * self.p
        self.far = lax.rem(self.c + 2, 4)
        self.near = self.c + 1 - 2 * lax.rem(self.c, 2)
        self.leads = self.q == 0
        self.follows = self.q >= 1
        self.passes = self.q + 1 < self.n_pos

    def barrier(self):
        sem = pltpu.get_barrier_semaphore()

        def greet(row, col):
            pl.semaphore_signal(sem, inc=1, device_id=(row, col), device_id_type=MESH)

        for i in range(1, self.n_cols):
            greet(self.r, lax.rem(self.c + i, self.n_cols))
        greet(self.partner, self.c)

        @pl.when(self.leads)
        def _():
            for s in range(1, self.n_pos):
                greet(self.r + 2 * s, self.c)
            for i in range(1, self.n_cols):
                greet(self.r + 2, lax.rem(self.c + i, self.n_cols))
            pl.semaphore_wait(sem, 2 * self.n_cols + self.n_pos - 2)

        @pl.when(self.follows)
        def _():
            greet(self.p, self.c)

            @pl.when(self.q == 1)
            def _():
                for i in range(1, self.n_cols):
                    greet(self.p, lax.rem(self.c + i, self.n_cols))

            @pl.when(self.q >= 2)
            def _():
                greet(self.r - 2, self.c)

            @pl.when(self.passes)
            def _():
                greet(self.r + 2, self.c)

            first = (self.q == 1).astype(jnp.int32)
            extra = first * (self.n_cols - 1) + (1 - first) + self.passes.astype(jnp.int32)
            pl.semaphore_wait(sem, self.n_cols + 1 + extra)


class Blocks:
    def __init__(self, at, lower, pieces, sems):
        self.at, self.lower, self.pieces = at, lower, pieces
        self.row_send, self.row_recv, self.near_send, self.near_recv = sems

    def of(self, k):
        return [i for i, piece in enumerate(self.pieces) if piece[3] == k]

    def half(self, piece, owner):
        _, lo, size, k = self.pieces[piece]
        start = pl.multiple_of(lo + owner * (size // 2), 8)
        return self.lower.at[k, pl.ds(start, size // 2), :]

    def place(self, piece):
        return self.half(piece, lax.rem(self.at.c, 2))

    def to_row(self, piece, row):
        spot = self.place(piece)
        return remote(spot, spot, self.row_send.at[piece], self.row_recv.at[piece], row, self.at.c)

    def to_near(self, piece):
        spot = self.place(piece)
        return remote(spot, spot, self.near_send.at[piece], self.near_recv.at[piece], self.at.r, self.at.near)

    def near_in(self, piece):
        spot = self.half(piece, 1 - lax.rem(self.at.c, 2))
        return remote(spot, spot, self.near_send.at[piece], self.near_recv.at[piece], self.at.r, self.at.near)


class Raw(Blocks):
    def send(self, k):
        for piece in self.of(k):

            @pl.when(self.at.r == self.pieces[piece][0])
            def _():
                self.to_row(piece, self.at.partner).start()

    def come(self, piece):
        @pl.when(self.at.p != self.pieces[piece][0])
        def _():
            self.to_row(piece, self.at.partner).wait_recv()
            self.to_near(piece).start()

    def done(self, piece):
        @pl.when(self.at.p != self.pieces[piece][0])
        def _():
            self.near_in(piece).wait_recv()
            self.to_near(piece).wait_send()

        @pl.when(self.at.p == self.pieces[piece][0])
        def _():
            self.to_row(piece, self.at.partner).wait_send()


class Solved(Blocks):
    def __init__(self, at, lower, pieces, sems, straight, n_straight):
        super().__init__(at, lower, pieces, sems)
        self.straight = straight
        self.first_straight = len(pieces) - n_straight

    def is_last(self, piece):
        return piece >= self.first_straight

    def sends(self, piece):
        if not self.is_last(piece):
            return [self.to_row(piece, self.at.r + 2)]
        spot = self.place(piece)
        return [
            remote(spot, spot, self.straight.at[piece - self.first_straight, s - 1], self.row_recv.at[piece], self.at.r + 2 * s, self.at.c)
            for s in reversed(range(1, self.at.n_pos))
        ]

    def send(self, piece):
        for copy in self.sends(piece):
            copy.start()

    def sent(self, piece):
        for copy in self.sends(piece):
            copy.wait_send()

    def take(self, piece):
        self.to_row(piece, self.at.r + 2).wait_recv()
        if not self.is_last(piece):

            @pl.when(self.at.passes)
            def _():
                self.to_row(piece, self.at.r + 2).start()

        self.to_near(piece).start()

    def taken(self, piece):
        self.near_in(piece).wait_recv()

    def finish(self):
        for piece in range(len(self.pieces)):
            self.to_near(piece).wait_send()
            if not self.is_last(piece):

                @pl.when(self.at.passes)
                def _():
                    self.to_row(piece, self.at.r + 2).wait_send()


class Rows:
    def __init__(self, at, panel, own, target, gathered, staged, sems):
        self.at, self.panel, self.own, self.target = at, panel, own, target
        self.gathered, self.staged = gathered, staged
        (self.dn_send, self.dn_recv, self.up_send, self.up_recv, self.x_send, self.x_recv,
         self.t_send, self.t_recv, self.l_send, self.l_recv) = sems
        self.width = panel.shape[0]
        self.share = self.width // at.n_cols
        self.chunk = self.share // CHUNKS

    def part(self, ref, m, owner=None):
        owner = self.at.c if owner is None else owner
        start = pl.multiple_of(owner * self.share + m * self.chunk, 8)
        return ref.at[pl.ds(start, self.chunk), :]

    def chain(self, kind, s, m):
        at = self.at
        if kind == "dn":
            origin, dest, send, recv = at.r + 2 * (s - 1), at.r - 2, self.dn_send, self.dn_recv
        else:
            origin, dest, send, recv = at.r - 2 * (s - 1), at.r + 2, self.up_send, self.up_recv
        spot = self.gathered[m].at[origin]
        src = self.part(self.panel, m) if s == 1 else spot
        return remote(src, spot, send.at[s - 1, m], recv.at[s - 1, m], dest, at.c)

    def awaited(self, kind, s, m):
        at = self.at
        recv, send = (self.dn_recv, self.dn_send) if kind == "dn" else (self.up_recv, self.up_send)
        spot = self.gathered[m].at[at.r + 2 * s if kind == "dn" else at.r - 2 * s]
        return remote(spot, spot, send.at[s - 1, m], recv.at[s - 1, m], at.r, at.c)

    def across(self, origin, m, own):
        at = self.at
        spot = self.gathered[m].at[2 * origin + at.p]
        src = self.part(self.panel, m) if own else spot
        return remote(src, spot, self.x_send.at[origin, m], self.x_recv.at[origin, m], at.partner, at.c)

    def crossed(self, origin, m):
        at = self.at
        spot = self.gathered[m].at[2 * origin + 1 - at.p]
        return remote(spot, spot, self.x_send.at[origin, m], self.x_recv.at[origin, m], at.r, at.c)

    def open(self):
        at = self.at
        for m in range(CHUNKS):

            @pl.when(at.q >= 2)
            def _():
                self.chain("dn", 1, m).start()

            @pl.when(at.passes)
            def _():
                self.chain("up", 1, m).start()

    def keep_own(self):
        for m in range(CHUNKS):
            start = pl.multiple_of(self.at.c * self.share + m * self.chunk, 8)
            self.gathered[m][self.at.r] = self.own[pl.ds(start, self.chunk), :]

    def relay(self, s, m):
        at = self.at

        @pl.when(at.q + s < at.n_pos)
        def _():
            self.awaited("dn", s, m).wait_recv()

            @pl.when(at.q >= 2)
            def _():
                self.chain("dn", s + 1, m).start()

        @pl.when(at.q - s >= 1)
        def _():
            self.awaited("up", s, m).wait_recv()

            @pl.when(at.passes)
            def _():
                self.chain("up", s + 1, m).start()

    def cross(self, s, m):
        at = self.at
        if s == 0:
            self.across(at.q, m, True).start()
            return

        @pl.when(at.q + s < at.n_pos)
        def _():
            self.across(at.q + s, m, False).start()

        @pl.when(at.q - s >= 1)
        def _():
            self.across(at.q - s, m, False).start()

    def select(self, m, rows, live):
        at = self.at
        for origin in range(1, at.n_pos):
            self.crossed(origin, m).wait_recv()
        start = pl.multiple_of(at.c * self.share + m * self.chunk, 8)
        for t in range(at.n_cols):
            value = self.gathered[m][rows[t]] * live[rows[t]].astype(jnp.float32)
            self.staged[m][t] = value

            @pl.when(at.c == t)
            def _():
                self.target[pl.ds(start, self.chunk), :] = value

    def deal(self, t, m):
        at = self.at
        return remote(self.staged[m].at[t], self.part(self.target, m), self.t_send.at[t, m],
                      self.t_recv.at[at.c, m], at.r, t)

    def deal_all(self, m):
        for t in range(self.at.n_cols):

            @pl.when(self.at.c != t)
            def _():
                self.deal(t, m).start()

            @pl.when(self.at.q == 1)
            def _():
                self.to_leader(t, m).start()

    def to_leader(self, t, m):
        at = self.at
        cols = pl.ds(pl.multiple_of(at.p * self.width, LEAF), self.width)
        return remote(self.staged[m].at[t, :, cols], self.left_part(m, at.c), self.l_send.at[t, m],
                      self.l_recv.at[at.c, m], at.p, t)

    def left_part(self, m, owner):
        start = pl.multiple_of(owner * self.share + m * self.chunk, 8)
        return self.target.at[pl.ds(start, self.chunk), pl.ds(0, self.width)]

    def dealt(self, m):
        at = self.at
        for i in range(1, at.n_cols):
            src = lax.rem(at.c + i, at.n_cols)
            spot = self.part(self.target, m, src)
            remote(spot, spot, self.t_send.at[src, m], self.t_recv.at[src, m], at.r, src).wait_recv()

    def arrived(self):
        for m in range(CHUNKS):
            for owner in range(self.at.n_cols):
                spot = self.left_part(m, owner)
                remote(spot, spot, self.l_send.at[owner, m], self.l_recv.at[owner, m],
                       self.at.r, self.at.c).wait_recv()

    def finish(self):
        at = self.at
        for m in range(CHUNKS):
            for t in range(at.n_cols):

                @pl.when(at.c != t)
                def _():
                    self.deal(t, m).wait_send()

                @pl.when(at.q == 1)
                def _():
                    self.to_leader(t, m).wait_send()

            for s in range(1, at.n_pos - 1):

                @pl.when((at.q >= 2) & (at.q + s - 1 < at.n_pos))
                def _():
                    self.chain("dn", s, m).wait_send()

                @pl.when(at.passes & (at.q - s + 1 >= 1))
                def _():
                    self.chain("up", s, m).wait_send()

            for origin in range(1, at.n_pos):
                self.across(origin, m, False).wait_send()


def lead(at, raw, solved, inverted, lower, split, inverses, aug, upper):
    total = lower.shape[1]
    n_leaf = total // LEAF
    rows = lax.broadcasted_iota(jnp.int32, (LEAF, LEAF), 0)
    lanes = lax.broadcasted_iota(jnp.int32, (LEAF, LEAF), 1)

    for b in range(1, n_leaf):
        lower[b, : b * LEAF, :] = jnp.zeros((b * LEAF, LEAF), jnp.float32)
    first = raw.of(0)
    raw.come(first[0])
    raw.done(first[0])

    def mirror(b):
        block = lower[b, b * LEAF : (b + 1) * LEAF, :]
        lower[b, b * LEAF : (b + 1) * LEAF, :] = jnp.where(rows >= lanes, block, block.T)

    def step(k, carry):
        here = pl.ds(pl.multiple_of(k * LEAF, LEAF), LEAF)
        aug[:, :LEAF] = lower[k, here, :]
        aug[:, LEAF:] = jnp.where(rows == lanes, 1.0, 0.0)
        factor_leaf(aug, upper, inverses.at[k])
        for b in range(n_leaf):

            @pl.when(k == b)
            def _():
                inverted.send(b)
                if b == 0:
                    for piece in first[1:] + raw.of(1) + raw.of(2):
                        raw.come(piece)
                    for piece in first[1:] + raw.of(1):
                        raw.done(piece)
                else:
                    if b + 2 < n_leaf:
                        for piece in raw.of(b + 2):
                            raw.come(piece)
                    if b + 1 < n_leaf:
                        for piece in raw.of(b + 1):
                            raw.done(piece)
                lo, hi = b * LEAF, (b + 1) * LEAF
                if hi < total:
                    column = times_trans(lower[b, hi:, :], inverses[b])
                    lower[b, hi:, :] = column
                    split.put(slice(hi, total), slice(lo, hi), column)
                    nxt = hi + LEAF
                    mirror(b + 1)
                    lower[b + 1, hi:, :] = lower[b + 1, hi:, :] - product(
                        split.get(slice(hi, total), slice(0, hi)), split.get(slice(hi, nxt), slice(0, hi)))
                    solved.send(b)

        lower[k, here, :] = upper[...].T
        return carry

    mirror(0)
    lax.fori_loop(0, n_leaf, step, 0)


def window_kernel(n_rows, n_cols, rows_in, live_in, panel, window, factor, other, updated,
                  window_rows, row_live, own, lower, target, inverses, aug, upper,
                  low_high, low_low, x_high, x_low, j_high, j_low, *rest):
    gathered, staged = rest[:CHUNKS], rest[CHUNKS : 2 * CHUNKS]
    own_sem, window_sem, rows_sem, live_sem, block_sem = rest[2 * CHUNKS : 2 * CHUNKS + 5]
    sems = rest[2 * CHUNKS + 5 :]
    at = Place(n_rows, n_cols)
    width = panel.shape[0]
    total = lower.shape[1]
    n_leaf = total // LEAF
    per = width // LEAF
    raw_pieces = [(0, 0, LEAF, 0), (0, LEAF, width - LEAF, 0)] + [
        (which, which * width + max(0, k - which * per) * LEAF, width - max(0, k - which * per) * LEAF, k)
        for k in range(n_leaf) for which in range(2) if k < (which + 1) * per and (k, which) != (0, 0)
    ]
    low_pieces = [(0, (k + 1) * LEAF, total - (k + 1) * LEAF, k) for k in range(n_leaf - 1)]
    raw = Raw(at, lower, raw_pieces, sems[2:6])
    solved = Solved(at, lower, low_pieces, sems[6:10], sems[1], LOW_STRAIGHT)
    inv_pieces = [(0, 0, LEAF, k) for k in range(n_leaf)]
    inverted = Solved(at, inverses, inv_pieces, sems[10:14], sems[0], INV_STRAIGHT)
    low_split, x_split = Split(low_high, low_low), Split(x_high, x_low)
    net = Rows(at, panel, own, target, gathered, staged, sems[14:])
    fetches = [
        pltpu.make_async_copy(window, updated, window_sem),
        pltpu.make_async_copy(rows_in, window_rows, rows_sem),
        pltpu.make_async_copy(live_in, row_live, live_sem),
    ]
    keep = pltpu.make_async_copy(panel, own, own_sem)

    def block_fetch(k):
        return pltpu.make_async_copy(
            panel.at[:, pl.ds(k * LEAF, LEAF)],
            lower.at[k, pl.ds(pl.multiple_of(at.p * width, LEAF), width), :], block_sem.at[k])

    @pl.when(at.leads)
    def _():
        for k in range(n_leaf):

            @pl.when(k < (at.p + 1) * per)
            def _():
                block_fetch(k).start()

    @pl.when(at.follows)
    def _():
        keep.start()

    for fetch in fetches:
        fetch.start()
    at.barrier()

    @pl.when(at.follows)
    def _():
        net.open()
        keep.wait()

    @pl.when(at.leads)
    def _():
        for k in range(n_leaf):

            @pl.when(k < (at.p + 1) * per)
            def _():
                block_fetch(k).wait()
                raw.send(k)

    for fetch in fetches:
        fetch.wait()
    live = row_live[at.r].astype(jnp.float32)

    @pl.when(at.leads)
    def _():
        lead(at, raw, solved, inverted, lower, low_split, inverses, aug, upper)
        for k in range(n_leaf):
            factor[:, k * LEAF : (k + 1) * LEAF] = lower[k, pl.ds(pl.multiple_of(at.p * width, width), width), :]
        for b in range(n_leaf):
            inverted.sent(b)
        for b in range(n_leaf - 1):
            solved.sent(b)
        net.arrived()
        updated[...] = updated[...] - target[:, :width].T

    @pl.when(at.follows)
    def _():
        net.keep_own()

        full = slice(0, width)
        j_split = Split(j_high, j_low)

        def span(b, count=1):
            return slice(b * LEAF, (b + count) * LEAF)

        def store(dst, split, b, value):
            dst[:, span(b)] = value
            split.put(full, span(b), value)

        share = width // n_cols
        halves_of = [[slice(c * share + h * share // 2, c * share + (h + 1) * share // 2) for c in range(n_cols)]
                     for h in range(2)]

        def gather(ref, h, cols):
            return jnp.concatenate([ref[rows, cols] for rows in halves_of[h]], axis=0)

        def scatter(ref, h, cols, value):
            size = share // 2
            for i, rows in enumerate(halves_of[h]):
                ref[rows, cols] = value[i * size : (i + 1) * size]

        def keep_j(h, b, value):
            scatter(other, h, span(b), value)
            for ref, part in zip((j_high, j_low), halves(value)):
                scatter(ref, h, span(b), part)

        def window_rows_step(h, k):
            def j_get(cols):
                return gather(j_high, h, cols), gather(j_low, h, cols)

            left, right = gather(target, h, span(k)), gather(target, h, span(k + 1))
            if k:
                both = product(j_get(span(0, k)), low_split.get(span(k, 2), span(0, k)))
                left, right = left - both[:, :LEAF], right - both[:, LEAF:]
            left = times_trans(left, inverses[k])
            keep_j(h, k, left)
            right = right - product(halves(left), low_split.get(span(k + 1), span(k)))
            if k + 2 < n_leaf:
                keep_j(h, k + 1, times_trans(right, inverses[k + 1]))
            else:
                scatter(other, h, span(k + 1), right)

        def cross(m):
            for s in range(at.n_pos - 2):
                net.cross(s, m)

        for b in range(n_leaf):
            if b == 0:
                for m in range(CHUNKS):
                    for s in range(1, at.n_pos - 2):
                        net.relay(s, m)
                    if m < EARLY:
                        cross(m)
            if b == n_leaf - 2:
                for k in range(0, n_leaf - 2, 2):
                    window_rows_step(0, k)
            for m in LATE.get(b, ()):
                net.relay(at.n_pos - 2, m)
                net.cross(at.n_pos - 2, m)
            if b and EARLY + b - 1 < CHUNKS:
                cross(EARLY + b - 1)
            for m in SELECT.get(b, ()):
                net.select(m, window_rows, row_live)
            if b + 1 < n_leaf:
                inverted.take(b)
            for m in SELECT.get(b, ()):
                net.deal_all(m)
            if b:
                solved.taken(b - 1)
                low_split.put(slice(b * LEAF, total), span(b - 1), lower[b - 1, b * LEAF :, :])
            if b % 2:
                now = factor[:, span(b)] - product(
                    x_split.get(full, span(b - 1)), low_split.get(span(b), span(b - 1)))
            else:
                pair = own[:, span(b, 2)] * live
                if b:
                    pair = pair - product(x_split.get(full, span(0, b)), low_split.get(span(b, 2), span(0, b)))
                now = pair[:, :LEAF]
                factor[:, span(b + 1)] = pair[:, LEAF:]
            for m in DEALT.get(b, ()):
                net.dealt(m)
            if b == n_leaf - 1:
                factor[:, span(b)] = now
                for k in range(0, n_leaf - 2, 2):
                    window_rows_step(1, k)
                window_rows_step(0, n_leaf - 2)
                window_rows_step(1, n_leaf - 2)
                updated[...] = updated[...] - product(x_split.get(full, span(0, b)), j_split.get(full, span(0, b)))
                now = factor[:, span(b)]
            if b + 1 == n_leaf:
                inverted.take(b)
            inverted.taken(b)
            now = times_trans(now, inverses[b])
            if b == n_leaf - 1:
                factor[:, span(b)] = now
                other[:, span(b)] = times_trans(other[:, span(b)], inverses[b])
            else:
                store(factor, x_split, b, now)
                solved.take(b)
        solved.finish()
        inverted.finish()
        net.finish()


def factor_window(window_rows, row_live, panel, window, n_rows, n_cols):
    if n_cols != 4 or n_rows < 6 or n_rows % 2:
        raise ValueError("unsupported mesh")
    width, total = panel.shape
    n_leaf = total // LEAF
    n_raw = n_leaf + width // LEAF + 1
    n_low = n_leaf - 1
    n_pos = n_rows // 2
    chunk = width // n_cols // CHUNKS
    dma = pltpu.SemaphoreType.DMA
    tall = jax.ShapeDtypeStruct(panel.shape, jnp.float32)
    return pl.pallas_call(
        functools.partial(window_kernel, n_rows, n_cols),
        out_shape=(tall, tall, jax.ShapeDtypeStruct(window.shape, jnp.float32)),
        in_specs=[pl.BlockSpec(memory_space=pltpu.HBM)] * 4,
        out_specs=(pl.BlockSpec(memory_space=pltpu.VMEM),) * 3,
        scratch_shapes=[
            pltpu.SMEM(window_rows.shape, jnp.int32),
            pltpu.SMEM(row_live.shape, jnp.int32),
            pltpu.VMEM(panel.shape, jnp.float32),
            pltpu.VMEM((n_leaf, total, LEAF), jnp.float32),
            pltpu.VMEM(panel.shape, jnp.float32),
            pltpu.VMEM((n_leaf, LEAF, LEAF), jnp.float32),
            pltpu.VMEM((LEAF, 2 * LEAF), jnp.float32),
            pltpu.VMEM((LEAF, LEAF), jnp.float32),
            pltpu.VMEM((total, total), jnp.bfloat16),
            pltpu.VMEM((total, total), jnp.bfloat16),
            pltpu.VMEM(panel.shape, jnp.bfloat16),
            pltpu.VMEM(panel.shape, jnp.bfloat16),
            pltpu.VMEM(panel.shape, jnp.bfloat16),
            pltpu.VMEM(panel.shape, jnp.bfloat16),
        ] + [pltpu.VMEM((n_rows, chunk, total), jnp.float32)] * CHUNKS
        + [pltpu.VMEM((n_cols, chunk, total), jnp.float32)] * CHUNKS
        + [
            dma(()), dma(()), dma(()), dma(()), dma((n_leaf,)),
            dma((INV_STRAIGHT, n_pos - 1)), dma((LOW_STRAIGHT, n_pos - 1)),
            dma((n_raw,)), dma((n_raw,)), dma((n_raw,)), dma((n_raw,)),
            dma((n_low,)), dma((n_low,)), dma((n_low,)), dma((n_low,)),
            dma((n_leaf,)), dma((n_leaf,)), dma((n_leaf,)), dma((n_leaf,)),
            dma((n_pos, CHUNKS)), dma((n_pos, CHUNKS)), dma((n_pos, CHUNKS)), dma((n_pos, CHUNKS)),
            dma((n_pos, CHUNKS)), dma((n_pos, CHUNKS)),
            dma((n_cols, CHUNKS)), dma((n_cols, CHUNKS)), dma((n_cols, CHUNKS)), dma((n_cols, CHUNKS)),
        ],
        compiler_params=pltpu.CompilerParams(
            collective_id=0, has_side_effects=True, vmem_limit_bytes=(29 << 20) + n_rows * n_cols * CHUNKS * chunk * total),
        cost_estimate=pl.CostEstimate(flops=10**10, bytes_accessed=10**7, transcendentals=0),
        name="factor_window",
    )(*[pltpu.with_memory_space_constraint(x, pltpu.HBM) for x in (window_rows, row_live, panel, window)])


def update_kernel(factor, other, partial, factor_out, updated, sem):
    store = pltpu.make_async_copy(factor, factor_out, sem)
    store.start()
    r = lax.axis_index("rows")
    lo = factor.shape[1] - LEAF

    @pl.when(r < P_SIZE)
    def _():
        updated[...] = partial[...]

    @pl.when(r >= P_SIZE)
    def _():
        updated[...] = partial[...] - times_trans(factor[:, lo:], other[:, lo:])

    store.wait()


def update_window(factor, other, partial):
    return pl.pallas_call(
        update_kernel,
        out_shape=(jax.ShapeDtypeStruct(factor.shape, jnp.float32),
                   jax.ShapeDtypeStruct(partial.shape, jnp.float32)),
        in_specs=[pl.BlockSpec(memory_space=pltpu.VMEM)] * 3,
        out_specs=(pl.BlockSpec(memory_space=pltpu.HBM), pl.BlockSpec(memory_space=pltpu.VMEM)),
        scratch_shapes=[pltpu.SemaphoreType.DMA(())],
        compiler_params=pltpu.CompilerParams(vmem_limit_bytes=24 << 20),
        cost_estimate=pl.CostEstimate(flops=10**9, bytes_accessed=10**7, transcendentals=0),
        name="update_window",
    )(factor, other, partial)


def shards(n_rows, n_cols, panel, window_block, row_live, window_rows):
    factor, other, partial = factor_window(window_rows, row_live, panel, window_block, n_rows, n_cols)
    return update_window(factor, other, partial)


def solution(mesh):
    in_specs = (P("rows", None), P("rows", "cols"), P(), P())
    out_specs = (P("rows", None), P("rows", "cols"))
    body = functools.partial(shards, mesh.shape["rows"], mesh.shape["cols"])
    return jax.shard_map(body, mesh=mesh, in_specs=in_specs, out_specs=out_specs, check_vma=False)
```
